1024 devices in a mesh: seq: 32 (over z, x_hi, core), head: 32 (over x_lo, y).
Axes of the slice: x: 8 (x_hi: 2, x_lo: 4; x = x_hi * 4 + x_lo), y: 8, z: 8, core: 2. Of those that a mesh axis runs over, the one named last changes fastest.
Arguments:
- queries: bfloat16 [4096, 128, 576], P('seq', 'head'), may hold values from -24 to 24
- latent_kv: bfloat16 [4096, 576], P('seq'), may hold values from -4.5 to 4.5
- grad_out: bfloat16 [4096, 128, 512], P('seq', 'head'), may hold values from -6 to 6
- doc_start: int32 [4096], P('seq'), may hold values from 0 to 4095, as said below
Outputs:
- grad_queries: bfloat16 [4096, 128, 576], P('seq', 'head')
- grad_latent: float32 [4096, 576], P('seq')
The draws below stay inside these ranges and needn't reach their ends.
Inputs may be any that keep to these rules, and one draw needn't show every extreme that they name: doc_start[p] is the first position of the document holding position p: it never falls along the sequence, doc_start[p] <= p, doc_start[0] = 0, every document holds at most 385 positions, and one document holds exactly 385.
All inputs are finite; a program needn't handle non-finite values.
Results may differ from the reference program's by a relative error of at most 0.0048.
Values may be sent and summed in bfloat16 or wider, within the bound.
No kernel may reach another device: no remote copies, remote signals or barrier semaphores. Data moves between devices by JAX's collectives and lax.ppermute only.
A program may use at most 32 MiB of HBM per device.

```python
import jax
import jax.numpy as jnp
from jax import lax

HEADS = 128
LAT = 512
KVW = 576
TOK_DEV = 128
REACH = 4
DOC_MAX = 385
SEQ_LEN = 4096
N_SEQ = 32


def document_starts(key):
    places = jnp.arange(SEQ_LEN, dtype=jnp.int32)
    lengths = jax.random.randint(jax.random.fold_in(key, 11), (SEQ_LEN,), 1, DOC_MAX + 1)
    chosen_doc = jax.random.randint(jax.random.fold_in(key, 12), (), 0, 2)
    lengths = jnp.where(places == chosen_doc, DOC_MAX, lengths)
    begins = jnp.cumsum(lengths) - lengths
    marks = jnp.zeros((SEQ_LEN,), jnp.int32).at[begins].max(1, mode='drop')
    start_marks = jnp.where((marks == 1) | (places == 0), places, 0)
    return lax.cummax(start_marks, axis=0)


def latent_base(key):
    return jnp.clip(jax.random.normal(jax.random.fold_in(key, 21), (SEQ_LEN, KVW), jnp.float32), -4.0, 4.0)


def draw_doc_start(key, part):
    return document_starts(key)


def draw_latent_kv(key, part):
    latent = latent_base(key)
    return latent.astype(jnp.bfloat16)


def draw_queries(key, part):
    gaussian = jax.random.normal(jax.random.fold_in(key, 31), (SEQ_LEN, HEADS, KVW), jnp.float32)
    return (0.4 * jnp.clip(gaussian, -6.0, 6.0)).astype(jnp.bfloat16)


def levels(stream_key, shape, cuts, low, high):
    gain = 1.0
    for dim, blocks in cuts:
        draws = jax.random.uniform(jax.random.fold_in(jax.random.fold_in(stream_key, 6), dim), (blocks,), jnp.float32, low / len(cuts), high / len(cuts))
        gain = gain * jnp.repeat(jnp.exp(draws), shape[dim] // blocks).reshape((-1,) + (1,) * (len(shape) - 1 - dim))
    return gain


def scatter_about(key, dims, deviation, reach, cuts=(), held_as=jnp.bfloat16):
    array = jax.random.normal(key, dims, jnp.float32) * deviation
    if len(cuts) > 0:
        array = levels(key, dims, cuts, -0.22, 0.18) * array
    return jnp.clip(array, min=-reach, max=reach).astype(held_as)


def setup_inputs(seed: int = 0) -> dict:
    splits = jax.random.split(jax.random.key(seed), 5)
    queries = draw_queries(jax.random.fold_in(splits[4], 71), 0)
    latent_kv = draw_latent_kv(jax.random.fold_in(splits[4], 71), 0)
    grad_out = scatter_about(splits[2], (SEQ_LEN, HEADS, LAT), 1.0, 6.0, ((0, 32), (1, 32)))
    doc_start = draw_doc_start(jax.random.fold_in(splits[4], 71), 0)
    return dict(queries=queries, latent_kv=latent_kv, grad_out=grad_out, doc_start=doc_start)


softmax_scale = 192.0 ** -0.5
lowest = -1.0e30
contract_first = (((0,), (0,)), ((), ()))
contract_last = (((1,), (1,)), ((), ()))


def reference(queries, latent_kv, grad_out, doc_start):
    margin = (REACH - 1) * TOK_DEV
    window = REACH * TOK_DEV
    kv_padded = jnp.concatenate([jnp.zeros((margin, KVW), jnp.bfloat16), latent_kv], axis=0)
    grad_padded = jnp.zeros((SEQ_LEN + margin, KVW), jnp.float32)

    def one_block(grad_pad, block_index):
        first = block_index * TOK_DEV
        query_rows = lax.dynamic_slice_in_dim(queries, first, TOK_DEV, 0).reshape(TOK_DEV * HEADS, KVW)
        grad_rows = lax.dynamic_slice_in_dim(grad_out, first, TOK_DEV, 0).reshape(TOK_DEV * HEADS, LAT)
        kv_block = lax.dynamic_slice_in_dim(kv_padded, first, window, 0)
        row_pos = jnp.repeat(first + jnp.arange(TOK_DEV, dtype=jnp.int32), HEADS)
        row_first = jnp.repeat(lax.dynamic_slice_in_dim(doc_start, first, TOK_DEV, 0), HEADS)
        key_pos = first - margin + jnp.arange(window, dtype=jnp.int32)
        visible = (key_pos[None, :] <= row_pos[:, None]) & (key_pos[None, :] >= row_first[:, None])
        scores = lax.dot_general(query_rows, kv_block, contract_last, preferred_element_type=jnp.float32) * softmax_scale
        row_top = jnp.max(jnp.where(visible, scores, lowest), axis=1)
        total_exp = jnp.sum(jnp.where(visible, jnp.exp(scores - row_top[:, None]), 0.0), axis=1)
        log_total = row_top + jnp.log(total_exp)
        probs = jnp.where(visible, jnp.exp(scores - log_total[:, None]), 0.0)
        grad_probs = lax.dot_general(grad_rows, kv_block[:, :LAT], contract_last, preferred_element_type=jnp.float32)
        delta = jnp.sum(probs * grad_probs, axis=1)
        grad_scores = (probs * (grad_probs - delta[:, None])).astype(jnp.bfloat16)
        probs_bf = probs.astype(jnp.bfloat16)
        grad_query = (jnp.dot(grad_scores, kv_block, preferred_element_type=jnp.float32) * softmax_scale).astype(jnp.bfloat16)
        from_scores = lax.dot_general(grad_scores, query_rows, contract_first, preferred_element_type=jnp.float32) * softmax_scale
        from_values = lax.dot_general(probs_bf, grad_rows, contract_first, preferred_element_type=jnp.float32)
        term = jnp.concatenate([from_scores[:, :LAT] + from_values, from_scores[:, LAT:]], axis=1)
        old = lax.dynamic_slice_in_dim(grad_pad, first, window, 0)
        grad_pad = lax.dynamic_update_slice_in_dim(grad_pad, old + term, first, 0)
        return grad_pad, grad_query.reshape(TOK_DEV, HEADS, KVW)

    grad_padded, grad_blocks = lax.scan(one_block, grad_padded, jnp.arange(N_SEQ, dtype=jnp.int32))
    grad_queries = grad_blocks.reshape(SEQ_LEN, HEADS, KVW)
    return (grad_queries, grad_padded[margin:])
```

```python
from functools import partial

import jax
import jax.numpy as jnp
from jax import lax
from jax.experimental import pallas as pl
from jax.experimental.pallas import tpu as pltpu
from jax.sharding import Mesh
from jax.sharding import PartitionSpec as P

LAT = 512
KVW = 576
TOK = 128
HEADS = 4
ROWS = TOK * HEADS
PART = 72
SEQ = ("z", "xh", "core")
RING = ("xh", "xl")

softmax_scale = 192.0 ** (-0.5)
lowest = -1e30
whole = pl.BlockSpec(memory_space=pltpu.VMEM)
scalars = pl.BlockSpec(memory_space=pltpu.SMEM)


def f32_dot(a, b):
    return jnp.dot(a, b, preferred_element_type=jnp.float32)


def attention_kernel(
    place, doc_ref, q_ref, qt_ref, g_ref, gt_ref, own_ref, px_ref, p2_ref, sw_ref,
    keep_ref, send_ref, ds_ref, kv_ref, bias_ref, p_ref,
):
    seq = place[0]
    core = lax.rem(seq, 2)
    for slot, ref in enumerate((own_ref, px_ref, p2_ref, sw_ref)):
        kv_ref[:, slot * TOK : (slot + 1) * TOK] = ref[...]
    first = jnp.broadcast_to(doc_ref[...].astype(jnp.float32), (TOK, TOK)).T
    row = lax.broadcasted_iota(jnp.int32, (TOK, TOK), 0)
    lane = lax.broadcasted_iota(jnp.int32, (TOK, TOK), 1)
    for slot, back in enumerate((0, 3 - 2 * core, 2, 1 + 2 * core)):
        key = lane + (seq - back) * TOK
        seen = (key <= row + seq * TOK) & (key.astype(jnp.float32) >= first)
        bias_ref[:, slot * TOK : (slot + 1) * TOK] = jnp.where(seen, 0.0, lowest)
    for head in range(HEADS):
        rows = slice(head * TOK, (head + 1) * TOK)
        scores = f32_dot(q_ref[rows, :], kv_ref[...]) * softmax_scale + bias_ref[...]
        grad_probs = f32_dot(g_ref[rows, :], kv_ref[:LAT, :])
        top = jnp.max(scores, axis=1, keepdims=True)
        exps = jnp.exp(scores - top)
        inverse = 1.0 / jnp.sum(exps, axis=1, keepdims=True)
        delta = jnp.sum(exps * grad_probs, axis=1, keepdims=True) * inverse
        probs = exps * inverse
        p_ref[rows, :] = probs.astype(jnp.bfloat16)
        ds_ref[rows, :] = (probs * (grad_probs - delta)).astype(jnp.bfloat16)
    for part in range(KVW // PART):
        cols = slice(part * PART, (part + 1) * PART)
        term = f32_dot(qt_ref[cols, :], ds_ref[...]) * softmax_scale
        term = term + f32_dot(gt_ref[cols, :], p_ref[...])
        keep_ref[0, part] = term[:, 0 * TOK : 1 * TOK]
        send_ref[0, part] = term[:, 1 * TOK : 2 * TOK].astype(jnp.bfloat16)
        keep_ref[1, part] = term[:, 2 * TOK : 3 * TOK]
        send_ref[1, part] = term[:, 3 * TOK : 4 * TOK].astype(jnp.bfloat16)


def attention(place, doc, q, qt, g, gt, own, px, p2, sw):
    parts = KVW // PART
    return pl.pallas_call(
        attention_kernel,
        out_shape=(
            jax.ShapeDtypeStruct((2, parts, PART, TOK), jnp.float32),
            jax.ShapeDtypeStruct((2, parts, PART, TOK), jnp.bfloat16),
            jax.ShapeDtypeStruct((ROWS, 4 * TOK), jnp.bfloat16),
        ),
        in_specs=[scalars] + [whole] * 9,
        out_specs=(whole, whole, whole),
        scratch_shapes=[
            pltpu.VMEM((KVW, 4 * TOK), jnp.bfloat16),
            pltpu.VMEM((TOK, 4 * TOK), jnp.float32),
            pltpu.VMEM((ROWS, 4 * TOK), jnp.bfloat16),
        ],
        cost_estimate=pl.CostEstimate(
            flops=4 * 2 * ROWS * 4 * TOK * KVW, bytes_accessed=6 << 20, transcendentals=ROWS * 4 * TOK
        ),
        compiler_params=pltpu.CompilerParams(vmem_limit_bytes=24 << 20),
        name="attention",
    )(place, doc, q, qt, g, gt, own, px, p2, sw)


def queries_kernel(ds_ref, own_ref, px_ref, p2_ref, sw_ref, out_ref, kv_ref):
    for slot, ref in enumerate((own_ref, px_ref, p2_ref, sw_ref)):
        kv_ref[:, slot * TOK : (slot + 1) * TOK] = ref[...]
    for head in range(HEADS):
        rows = slice(head * TOK, (head + 1) * TOK)
        total = lax.dot_general(
            kv_ref[...], ds_ref[rows, :], (((1,), (1,)), ((), ())), preferred_element_type=jnp.float32
        )
        out_ref[head] = (total * softmax_scale).astype(jnp.bfloat16)


def query_grads(ds, own, px, p2, sw):
    return pl.pallas_call(
        queries_kernel,
        out_shape=jax.ShapeDtypeStruct((HEADS, KVW, TOK), jnp.bfloat16),
        in_specs=[whole] * 5,
        out_specs=whole,
        scratch_shapes=[pltpu.VMEM((KVW, 4 * TOK), jnp.bfloat16)],
        cost_estimate=pl.CostEstimate(
            flops=2 * ROWS * 4 * TOK * KVW, bytes_accessed=2 << 20, transcendentals=0
        ),
        compiler_params=pltpu.CompilerParams(vmem_limit_bytes=12 << 20),
        name="query_grads",
    )(ds, own, px, p2, sw)


def join_kernel(core_ref, keep_ref, came_ref, out_ref):
    even = core_ref[0] == 0
    for part in range(KVW // PART):
        side = came_ref[0, part].astype(jnp.float32)
        zero = jnp.zeros_like(side)
        out_ref[part, 0] = (keep_ref[0, part] + jnp.where(even, side, zero)).astype(jnp.bfloat16)
        out_ref[part, 1] = (keep_ref[1, part] + came_ref[1, part].astype(jnp.float32)).astype(
            jnp.bfloat16
        )
        out_ref[part, 2] = jnp.where(even, zero, side).astype(jnp.bfloat16)


def join_cores(core, keep, came):
    return pl.pallas_call(
        join_kernel,
        out_shape=jax.ShapeDtypeStruct((KVW // PART, 3, PART, TOK), jnp.bfloat16),
        in_specs=[scalars, whole, whole],
        out_specs=whole,
        cost_estimate=pl.CostEstimate(flops=1 << 20, bytes_accessed=2 << 20, transcendentals=0),
        compiler_params=pltpu.CompilerParams(vmem_limit_bytes=8 << 20),
        name="join_cores",
    )(core, keep, came)


def per_device(queries, latent_kv, grad_out, doc_start):
    tokens, _, width = queries.shape
    count = lax.axis_size(SEQ)
    seq = lax.axis_index(SEQ).astype(jnp.int32)
    core = lax.axis_index("core").astype(jnp.int32)
    half = lax.axis_index("xh")

    own = latent_kv.T
    p2 = lax.ppermute(own, SEQ, [(i, i + 2) for i in range(count - 2)])
    mixed = [(i, i + 1 + 2 * (i % 2)) for i in range(count)]
    px = lax.ppermute(own, SEQ, [(a, b) for a, b in mixed if b < count])
    sw = lax.ppermute(p2, "core", [(0, 1), (1, 0)])

    q = queries.transpose(1, 0, 2).reshape(ROWS, width)
    qt = queries.transpose(2, 1, 0).reshape(width, ROWS)
    g = grad_out.transpose(1, 0, 2).reshape(ROWS, LAT)
    gt = jnp.pad(grad_out.transpose(2, 1, 0).reshape(LAT, ROWS), ((0, width - LAT), (0, 0)))

    keep, send, ds = attention(
        seq.reshape(1), doc_start.reshape(1, tokens), q, qt, g, gt, own, px, p2, sw
    )
    came = lax.ppermute(send, "core", [(0, 1), (1, 0)])
    terms = join_cores(core.reshape(1), keep, came)
    here = lax.all_to_all(terms, "y", 0, 0, tiled=True).astype(jnp.float32).sum(axis=0)

    low = half == 0
    nothing = jnp.zeros_like(here[0])
    cross = jnp.stack([jnp.where(low, here[2], nothing), jnp.where(low, here[1], here[2])])
    planes = lax.axis_size("z")
    below = lax.ppermute(cross, "z", [(i, i - 1) for i in range(1, planes)])
    plane = below + jnp.stack([jnp.where(low, here[0], here[1]), jnp.where(low, nothing, here[0])])
    plane = plane.astype(jnp.bfloat16)
    spread = jnp.broadcast_to(plane[:, None], (2, 4, PART, tokens)).reshape(8, PART, tokens)
    mine = lax.all_to_all(spread, RING, 0, 0, tiled=True).astype(jnp.float32).sum(axis=0)
    mine = mine.astype(jnp.bfloat16)
    grad = lax.all_to_all(
        jnp.broadcast_to(mine[None], (8, PART, tokens)), "y", 0, 0, tiled=True
    )
    grad_latent = grad.astype(jnp.float32).reshape(width, tokens).T

    grad_queries = query_grads(ds, own, px, p2, sw).transpose(2, 0, 1)
    return grad_queries, grad_latent


def solution(mesh):
    fine = Mesh(mesh.devices.reshape(8, 2, 2, 4, 8), ("z", "xh", "core", "xl", "y"))
    head = ("xl", "y")
    in_specs = (P(SEQ, head, None), P(SEQ, None), P(SEQ, head, None), P(SEQ))
    out_specs = (P(SEQ, head, None), P(SEQ, None))
    return jax.shard_map(
        per_device, mesh=fine, in_specs=in_specs, out_specs=out_specs, check_vma=False
    )
```

```python
from functools import partial

import jax
import jax.numpy as jnp
from jax import lax
from jax.experimental import pallas as pl
from jax.experimental.pallas import tpu as pltpu
from jax.sharding import Mesh
from jax.sharding import PartitionSpec as P

LAT = 512
KVW = 576
TOK = 128
HEADS = 4
ROWS = TOK * HEADS
PART = 72
SEQ = ("z", "xh", "core")
RING = ("xh", "xl")

softmax_scale = 192.0 ** (-0.5)
lowest = -1e30
whole = pl.BlockSpec(memory_space=pltpu.VMEM)
scalars = pl.BlockSpec(memory_space=pltpu.SMEM)


def f32_dot(a, b):
    return jnp.dot(a, b, preferred_element_type=jnp.float32)


def attention_kernel(
    place, doc_ref, q_ref, qt_ref, g_ref, gt_ref, own_ref, px_ref, p2_ref, sw_ref,
    term_ref, ds_ref, kv_ref, bias_ref, p_ref,
):
    seq = place[0]
    core = lax.rem(seq, 2)
    for slot, ref in enumerate((own_ref, px_ref, p2_ref, sw_ref)):
        kv_ref[:, slot * TOK : (slot + 1) * TOK] = ref[...]
    first = jnp.broadcast_to(doc_ref[...], (TOK, TOK)).T
    row = lax.broadcasted_iota(jnp.int32, (TOK, TOK), 0)
    lane = lax.broadcasted_iota(jnp.int32, (TOK, TOK), 1)
    for slot, back in enumerate((0, 3 - 2 * core, 2, 1 + 2 * core)):
        key = lane + (seq - back) * TOK
        seen = (key <= row + seq * TOK) & (key.astype(jnp.float32) >= first)
        bias_ref[:, slot * TOK : (slot + 1) * TOK] = jnp.where(seen, 0.0, lowest)
    for head in range(HEADS):
        rows = slice(head * TOK, (head + 1) * TOK)
        scores = f32_dot(q_ref[rows, :], kv_ref[...]) * softmax_scale + bias_ref[...]
        grad_probs = f32_dot(g_ref[rows, :], kv_ref[:LAT, :])
        top = jnp.max(scores, axis=1, keepdims=True)
        exps = jnp.exp(scores - top)
        inverse = 1.0 / jnp.sum(exps, axis=1, keepdims=True)
        delta = jnp.sum(exps * grad_probs, axis=1, keepdims=True) * inverse
        probs = exps * inverse
        p_ref[rows, :] = probs.astype(jnp.bfloat16)
        ds_ref[rows, :] = (probs * (grad_probs - delta)).astype(jnp.bfloat16)
    for part in range(KVW // PART):
        cols = slice(part * PART, (part + 1) * PART)
        term = f32_dot(qt_ref[cols, :], ds_ref[...]) * softmax_scale
        term = (term + f32_dot(gt_ref[cols, :], p_ref[...])).astype(jnp.bfloat16)
        same, other = core, 1 - core
        term_ref[same, part, 0] = term[:, 0 * TOK : 1 * TOK]
        term_ref[other, part, 0] = term[:, 1 * TOK : 2 * TOK]
        term_ref[same, part, 1] = term[:, 2 * TOK : 3 * TOK]
        term_ref[other, part, 1] = term[:, 3 * TOK : 4 * TOK]


def attention(place, doc, q, qt, g, gt, own, px, p2, sw):
    return pl.pallas_call(
        attention_kernel,
        out_shape=(
            jax.ShapeDtypeStruct((2, KVW // PART, 2, PART, TOK), jnp.bfloat16),
            jax.ShapeDtypeStruct((ROWS, 4 * TOK), jnp.bfloat16),
        ),
        in_specs=[scalars] + [whole] * 9,
        out_specs=(whole, whole),
        scratch_shapes=[
            pltpu.VMEM((KVW, 4 * TOK), jnp.bfloat16),
            pltpu.VMEM((TOK, 4 * TOK), jnp.float32),
            pltpu.VMEM((ROWS, 4 * TOK), jnp.bfloat16),
        ],
        cost_estimate=pl.CostEstimate(
            flops=4 * 2 * ROWS * 4 * TOK * KVW, bytes_accessed=6 << 20, transcendentals=ROWS * 4 * TOK
        ),
        compiler_params=pltpu.CompilerParams(vmem_limit_bytes=24 << 20),
        name="attention",
    )(place, doc, q, qt, g, gt, own, px, p2, sw)


def queries_kernel(ds_ref, own_ref, px_ref, p2_ref, sw_ref, out_ref, kv_ref):
    for slot, ref in enumerate((own_ref, px_ref, p2_ref, sw_ref)):
        kv_ref[:, slot * TOK : (slot + 1) * TOK] = ref[...]
    for head in range(HEADS):
        rows = slice(head * TOK, (head + 1) * TOK)
        total = lax.dot_general(
            kv_ref[...], ds_ref[rows, :], (((1,), (1,)), ((), ())), preferred_element_type=jnp.float32
        )
        out_ref[head] = (total * softmax_scale).astype(jnp.bfloat16)


def query_grads(ds, own, px, p2, sw):
    return pl.pallas_call(
        queries_kernel,
        out_shape=jax.ShapeDtypeStruct((HEADS, KVW, TOK), jnp.bfloat16),
        in_specs=[whole] * 5,
        out_specs=whole,
        scratch_shapes=[pltpu.VMEM((KVW, 4 * TOK), jnp.bfloat16)],
        cost_estimate=pl.CostEstimate(
            flops=2 * ROWS * 4 * TOK * KVW, bytes_accessed=2 << 20, transcendentals=0
        ),
        compiler_params=pltpu.CompilerParams(vmem_limit_bytes=12 << 20),
        name="query_grads",
    )(ds, own, px, p2, sw)


def combine_kernel(place, came_ref, cross_ref, plane_ref):
    seq = place[0]
    even = lax.rem(seq, 2) == 0
    low = lax.rem(lax.div(seq, 2), 2) == 0
    parts = KVW // PART

    def summed(core, window):
        total = came_ref[core * parts, window].astype(jnp.float32)
        for part in range(1, parts):
            total = total + came_ref[core * parts + part, window].astype(jnp.float32)
        return total

    near, far = [summed(0, 0), summed(0, 1)], [summed(1, 0), summed(1, 1)]
    nothing = jnp.zeros((PART, TOK), jnp.float32)
    side = jnp.where(even, far[0], near[0])
    first = jnp.where(even, near[0], far[0]) + jnp.where(even, side, nothing)
    second = near[1] + far[1]
    third = jnp.where(even, nothing, side)
    cross_ref[0] = jnp.where(low, third, nothing)
    cross_ref[1] = jnp.where(low, second, third)
    plane_ref[0] = jnp.where(low, first, second)
    plane_ref[1] = jnp.where(low, nothing, first)


def combine(place, came):
    shape = jax.ShapeDtypeStruct((2, PART, TOK), jnp.float32)
    return pl.pallas_call(
        combine_kernel,
        out_shape=(shape, shape),
        in_specs=[scalars, whole],
        out_specs=(whole, whole),
        cost_estimate=pl.CostEstimate(flops=1 << 19, bytes_accessed=1 << 20, transcendentals=0),
        compiler_params=pltpu.CompilerParams(vmem_limit_bytes=8 << 20),
        name="combine",
    )(place, came)


def per_device(queries, latent_kv, grad_out, doc_start):
    tokens, _, width = queries.shape
    count = lax.axis_size(SEQ)
    seq = lax.axis_index(SEQ).astype(jnp.int32)

    own = latent_kv.T
    p2 = lax.ppermute(own, SEQ, [(i, i + 2) for i in range(count - 2)])
    mixed = [(i, i + 1 + 2 * (i % 2)) for i in range(count)]
    px = lax.ppermute(own, SEQ, [(a, b) for a, b in mixed if b < count])
    sw = lax.ppermute(p2, "core", [(0, 1), (1, 0)])

    q = queries.transpose(1, 0, 2).reshape(ROWS, width)
    qt = queries.transpose(2, 1, 0).reshape(width, ROWS)
    g = grad_out.transpose(1, 0, 2).reshape(ROWS, LAT)
    gt = jnp.pad(grad_out.transpose(2, 1, 0).reshape(LAT, ROWS), ((0, width - LAT), (0, 0)))

    doc = doc_start.astype(jnp.float32).reshape(1, tokens)
    place = seq.reshape(1)
    terms, ds = attention(place, doc, q, qt, g, gt, own, px, p2, sw)
    parts = width // PART
    came = lax.all_to_all(
        terms.reshape(2 * parts, 2, PART, tokens), ("core", "y"), 0, 0, tiled=True
    )
    cross, here = combine(place, came)
    ds, cross = lax.optimization_barrier((ds, cross))
    planes = lax.axis_size("z")
    below = lax.ppermute(cross, "z", [(i, i - 1) for i in range(1, planes)])
    plane = (below + here).astype(jnp.bfloat16)
    query_grad = query_grads(ds, own, px, p2, sw)
    plane, query_grad = lax.optimization_barrier((plane, query_grad))
    spread = jnp.broadcast_to(plane[:, None], (2, 4, PART, tokens)).reshape(8, PART, tokens)
    mine = lax.all_to_all(spread, RING, 0, 0, tiled=True).astype(jnp.float32).sum(axis=0)
    mine = mine.astype(jnp.bfloat16)
    grad = lax.all_to_all(
        jnp.broadcast_to(mine[None], (8, PART, tokens)), "y", 0, 0, tiled=True
    )
    grad_latent = grad.astype(jnp.float32).reshape(width, tokens).T
    return query_grad.transpose(2, 0, 1), grad_latent


def solution(mesh):
    fine = Mesh(mesh.devices.reshape(8, 2, 2, 4, 8), ("z", "xh", "core", "xl", "y"))
    head = ("xl", "y")
    in_specs = (P(SEQ, head, None), P(SEQ, None), P(SEQ, head, None), P(SEQ))
    out_specs = (P(SEQ, head, None), P(SEQ, None))
    return jax.shard_map(
        per_device, mesh=fine, in_specs=in_specs, out_specs=out_specs, check_vma=False
    )
```

```python
import jax
import jax.numpy as jnp
from jax import lax
from jax.experimental import pallas as pl
from jax.experimental.pallas import tpu as pltpu
from jax.sharding import Mesh
from jax.sharding import PartitionSpec as P

LAT = 512
KVW = 576
TOK = 128
HEADS = 4
ROWS = TOK * HEADS
PART = 72
SHARES = 32
SHARE = KVW // SHARES
SEQ = ("z", "xh", "core")
HEAD = ("xl", "y")

softmax_scale = 192.0 ** (-0.5)
lowest = -1e30
whole = pl.BlockSpec(memory_space=pltpu.VMEM)
scalars = pl.BlockSpec(memory_space=pltpu.SMEM)


def f32_dot(a, b):
    return jnp.dot(a, b, preferred_element_type=jnp.float32)


def attention_kernel(
    place, doc_ref, q_ref, qt_ref, g_ref, gt_ref, own_ref, px_ref, p2_ref, sw_ref,
    term_ref, ds_ref, kv_ref, bias_ref, p_ref, mixed_ref,
):
    seq = place[0]
    core = lax.rem(seq, 2)
    for slot, ref in enumerate((own_ref, px_ref, p2_ref, sw_ref)):
        kv_ref[:, slot * TOK : (slot + 1) * TOK] = ref[...]
    first = jnp.broadcast_to(doc_ref[...], (TOK, TOK)).T
    row = lax.broadcasted_iota(jnp.int32, (TOK, TOK), 0)
    lane = lax.broadcasted_iota(jnp.int32, (TOK, TOK), 1)
    for slot, back in enumerate((0, 3 - 2 * core, 2, 1 + 2 * core)):
        key = lane + (seq - back) * TOK
        seen = (key <= row + seq * TOK) & (key.astype(jnp.float32) >= first)
        bias_ref[:, slot * TOK : (slot + 1) * TOK] = jnp.where(seen, 0.0, lowest)
    for head in range(HEADS):
        rows = slice(head * TOK, (head + 1) * TOK)
        scores = f32_dot(q_ref[rows, :], kv_ref[...]) * softmax_scale + bias_ref[...]
        grad_probs = f32_dot(g_ref[rows, :], kv_ref[:LAT, :])
        top = jnp.max(scores, axis=1, keepdims=True)
        exps = jnp.exp(scores - top)
        inverse = 1.0 / jnp.sum(exps, axis=1, keepdims=True)
        delta = jnp.sum(exps * grad_probs, axis=1, keepdims=True) * inverse
        probs = exps * inverse
        p_ref[rows, :] = probs.astype(jnp.bfloat16)
        ds_ref[rows, :] = (probs * (grad_probs - delta)).astype(jnp.bfloat16)
    for part in range(KVW // PART):
        cols = slice(part * PART, (part + 1) * PART)
        term = f32_dot(qt_ref[cols, :], ds_ref[...]) * softmax_scale
        term = term + f32_dot(gt_ref[cols, :], p_ref[...])
        for slot in range(4):
            rows = pl.ds(4 * PART * part + slot, PART, stride=4)
            mixed_ref[rows, :] = term[:, slot * TOK : (slot + 1) * TOK]
    turn = lax.rem(lax.div(seq, 2), 2) * (SHARES // 2)
    for share in range(SHARES):
        rows = slice(4 * SHARE * share, 4 * SHARE * (share + 1))
        term_ref[lax.rem(share + turn, SHARES)] = mixed_ref[rows, :].astype(jnp.bfloat16)


def attention(place, doc, q, qt, g, gt, own, px, p2, sw):
    return pl.pallas_call(
        attention_kernel,
        out_shape=(
            jax.ShapeDtypeStruct((SHARES, 4 * SHARE, TOK), jnp.bfloat16),
            jax.ShapeDtypeStruct((ROWS, 4 * TOK), jnp.bfloat16),
        ),
        in_specs=[scalars] + [whole] * 9,
        out_specs=(whole, whole),
        scratch_shapes=[
            pltpu.VMEM((KVW, 4 * TOK), jnp.bfloat16),
            pltpu.VMEM((TOK, 4 * TOK), jnp.float32),
            pltpu.VMEM((ROWS, 4 * TOK), jnp.bfloat16),
            pltpu.VMEM((4 * KVW, TOK), jnp.float32),
        ],
        cost_estimate=pl.CostEstimate(
            flops=4 * 2 * ROWS * 4 * TOK * KVW, bytes_accessed=6 << 20, transcendentals=ROWS * 4 * TOK
        ),
        compiler_params=pltpu.CompilerParams(vmem_limit_bytes=24 << 20),
        name="attention",
    )(place, doc, q, qt, g, gt, own, px, p2, sw)


def queries_kernel(ds_ref, own_ref, px_ref, p2_ref, sw_ref, out_ref, kv_ref):
    for slot, ref in enumerate((own_ref, px_ref, p2_ref, sw_ref)):
        kv_ref[:, slot * TOK : (slot + 1) * TOK] = ref[...]
    for head in range(HEADS):
        rows = slice(head * TOK, (head + 1) * TOK)
        total = lax.dot_general(
            kv_ref[...], ds_ref[rows, :], (((1,), (1,)), ((), ())), preferred_element_type=jnp.float32
        )
        out_ref[head] = (total * softmax_scale).astype(jnp.bfloat16)


def query_grads(ds, own, px, p2, sw):
    return pl.pallas_call(
        queries_kernel,
        out_shape=jax.ShapeDtypeStruct((HEADS, KVW, TOK), jnp.bfloat16),
        in_specs=[whole] * 5,
        out_specs=whole,
        scratch_shapes=[pltpu.VMEM((KVW, 4 * TOK), jnp.bfloat16)],
        cost_estimate=pl.CostEstimate(
            flops=2 * ROWS * 4 * TOK * KVW, bytes_accessed=2 << 20, transcendentals=0
        ),
        compiler_params=pltpu.CompilerParams(vmem_limit_bytes=12 << 20),
        name="query_grads",
    )(ds, own, px, p2, sw)


def combine_kernel(came_ref, own_ref, px_ref, p2_ref, sw_ref, sum_ref):
    total = came_ref[0].astype(jnp.float32)
    for source in range(1, SHARES):
        total = total + came_ref[source].astype(jnp.float32)
    sum_ref[...] = total
    for slot, ref in enumerate((own_ref, px_ref, p2_ref, sw_ref)):
        ref[...] = sum_ref[pl.ds(slot, SHARE, stride=4), :]


def combine(came):
    shape = jax.ShapeDtypeStruct((SHARE, TOK), jnp.float32)
    return pl.pallas_call(
        combine_kernel,
        out_shape=(shape,) * 4,
        in_specs=[whole],
        out_specs=(whole,) * 4,
        scratch_shapes=[pltpu.VMEM((4 * SHARE, TOK), jnp.float32)],
        cost_estimate=pl.CostEstimate(flops=1 << 19, bytes_accessed=1 << 20, transcendentals=0),
        compiler_params=pltpu.CompilerParams(vmem_limit_bytes=8 << 20),
        name="combine",
    )(came)


def finish_kernel(place, came_ref, out_ref):
    turn = lax.rem(lax.div(place[0], 2), 2) * (SHARES // 2)
    for share in range(SHARES):
        rows = slice(SHARE * share, SHARE * (share + 1))
        out_ref[rows, :] = came_ref[lax.rem(share + turn, SHARES)].astype(jnp.float32)


def finish(place, came):
    return pl.pallas_call(
        finish_kernel,
        out_shape=jax.ShapeDtypeStruct((KVW, TOK), jnp.float32),
        in_specs=[scalars, whole],
        out_specs=whole,
        cost_estimate=pl.CostEstimate(flops=1 << 17, bytes_accessed=1 << 19, transcendentals=0),
        compiler_params=pltpu.CompilerParams(vmem_limit_bytes=8 << 20),
        name="finish",
    )(place, came)


def routes(count):
    across = SHARES // 2
    halo = [(i, i + 2, across) for i in range(count)]
    mixed = [(i, i + 1 + 2 * (i % 2), 0) for i in range(count)]
    turned = [(i, i + 3 - 2 * (i % 2), across) for i in range(count)]

    def pairs(moves, back):
        route = []
        for start, end, other in moves:
            if end < count:
                for head in range(SHARES):
                    pair = (start * SHARES + head, end * SHARES + (head ^ other))
                    route.append(pair[::-1] if back else pair)
        return route

    return pairs(halo, False), pairs(mixed, False), [pairs(m, True) for m in (mixed, halo, turned)]


def per_device(queries, latent_kv, grad_out, doc_start):
    tokens, _, width = queries.shape
    everyone = SEQ + HEAD
    halo, mixed, back = routes(lax.axis_size(SEQ))
    place = lax.axis_index(SEQ).astype(jnp.int32).reshape(1)

    own = latent_kv.T
    p2 = lax.ppermute(own, everyone, halo)
    px = lax.ppermute(own, everyone, mixed)
    sw = lax.ppermute(p2, "core", [(0, 1), (1, 0)])

    q = queries.transpose(1, 0, 2).reshape(ROWS, width)
    qt = queries.transpose(2, 1, 0).reshape(width, ROWS)
    g = grad_out.transpose(1, 0, 2).reshape(ROWS, LAT)
    gt = jnp.pad(grad_out.transpose(2, 1, 0).reshape(LAT, ROWS), ((0, width - LAT), (0, 0)))
    doc = doc_start.astype(jnp.float32).reshape(1, tokens)

    terms, ds = attention(place, doc, q, qt, g, gt, own, px, p2, sw)
    came = lax.all_to_all(terms, HEAD, 0, 0, tiled=True)
    mine, *others = combine(came)
    ds, mine, *others = lax.optimization_barrier((ds, mine, *others))
    for part, route in zip(others, back):
        mine = mine + lax.ppermute(part, everyone, route)
    query_grad = query_grads(ds, own, px, p2, sw)
    mine, query_grad = lax.optimization_barrier((mine.astype(jnp.bfloat16), query_grad))
    spread = jnp.broadcast_to(mine[None], (SHARES, SHARE, tokens))
    grad = lax.all_to_all(spread, HEAD, 0, 0, tiled=True)
    return query_grad.transpose(2, 0, 1), finish(place, grad).T


def solution(mesh):
    fine = Mesh(mesh.devices.reshape(8, 2, 2, 4, 8), ("z", "xh", "core", "xl", "y"))
    in_specs = (P(SEQ, HEAD, None), P(SEQ, None), P(SEQ, HEAD, None), P(SEQ))
    out_specs = (P(SEQ, HEAD, None), P(SEQ, None))
    return jax.shard_map(
        per_device, mesh=fine, in_specs=in_specs, out_specs=out_specs, check_vma=False
    )
```

```python
import jax
import jax.numpy as jnp
from jax import lax
from jax.experimental import pallas as pl
from jax.experimental.pallas import tpu as pltpu
from jax.sharding import Mesh
from jax.sharding import PartitionSpec as P

LAT = 512
KVW = 576
TOK = 128
HEADS = 4
ROWS = TOK * HEADS
PART = 72
SHARES = 32
SHARE = KVW // SHARES
SEQ = ("z", "xh", "core")
HEAD = ("xl", "y")

softmax_scale = 192.0 ** (-0.5)
lowest = -1e30
whole = pl.BlockSpec(memory_space=pltpu.VMEM)
scalars = pl.BlockSpec(memory_space=pltpu.SMEM)


def f32_dot(a, b):
    return jnp.dot(a, b, preferred_element_type=jnp.float32)


def attention_kernel(
    place, doc_ref, q_ref, qt_ref, g_ref, gt_ref, own_ref, px_ref, p2_ref, sw_ref,
    keep_ref, send_ref, ds_ref, kv_ref, bias_ref, p_ref,
):
    seq = place[0]
    core = lax.rem(seq, 2)
    for slot, ref in enumerate((own_ref, px_ref, p2_ref, sw_ref)):
        kv_ref[:, slot * TOK : (slot + 1) * TOK] = ref[...]
    first = jnp.broadcast_to(doc_ref[...], (TOK, TOK)).T
    row = lax.broadcasted_iota(jnp.int32, (TOK, TOK), 0)
    lane = lax.broadcasted_iota(jnp.int32, (TOK, TOK), 1)
    for slot, back in enumerate((0, 3 - 2 * core, 2, 1 + 2 * core)):
        key = lane + (seq - back) * TOK
        seen = (key <= row + seq * TOK) & (key.astype(jnp.float32) >= first)
        bias_ref[:, slot * TOK : (slot + 1) * TOK] = jnp.where(seen, 0.0, lowest)
    for head in range(HEADS):
        rows = slice(head * TOK, (head + 1) * TOK)
        scores = f32_dot(q_ref[rows, :], kv_ref[...]) * softmax_scale + bias_ref[...]
        grad_probs = f32_dot(g_ref[rows, :], kv_ref[:LAT, :])
        top = jnp.max(scores, axis=1, keepdims=True)
        exps = jnp.exp(scores - top)
        inverse = 1.0 / jnp.sum(exps, axis=1, keepdims=True)
        delta = jnp.sum(exps * grad_probs, axis=1, keepdims=True) * inverse
        probs = exps * inverse
        p_ref[rows, :] = probs.astype(jnp.bfloat16)
        ds_ref[rows, :] = (probs * (grad_probs - delta)).astype(jnp.bfloat16)
    for part in range(KVW // PART):
        cols = slice(part * PART, (part + 1) * PART)
        term = f32_dot(qt_ref[cols, :], ds_ref[...]) * softmax_scale
        term = term + f32_dot(gt_ref[cols, :], p_ref[...])
        keep_ref[0, cols, :] = term[:, 0 * TOK : 1 * TOK]
        send_ref[0, cols, :] = term[:, 1 * TOK : 2 * TOK].astype(jnp.bfloat16)
        keep_ref[1, cols, :] = term[:, 2 * TOK : 3 * TOK]
        send_ref[1, cols, :] = term[:, 3 * TOK : 4 * TOK].astype(jnp.bfloat16)


def attention(place, doc, q, qt, g, gt, own, px, p2, sw):
    return pl.pallas_call(
        attention_kernel,
        out_shape=(
            jax.ShapeDtypeStruct((2, KVW, TOK), jnp.float32),
            jax.ShapeDtypeStruct((2, KVW, TOK), jnp.bfloat16),
            jax.ShapeDtypeStruct((ROWS, 4 * TOK), jnp.bfloat16),
        ),
        in_specs=[scalars] + [whole] * 9,
        out_specs=(whole, whole, whole),
        scratch_shapes=[
            pltpu.VMEM((KVW, 4 * TOK), jnp.bfloat16),
            pltpu.VMEM((TOK, 4 * TOK), jnp.float32),
            pltpu.VMEM((ROWS, 4 * TOK), jnp.bfloat16),
        ],
        cost_estimate=pl.CostEstimate(
            flops=4 * 2 * ROWS * 4 * TOK * KVW, bytes_accessed=6 << 20, transcendentals=ROWS * 4 * TOK
        ),
        compiler_params=pltpu.CompilerParams(vmem_limit_bytes=24 << 20),
        name="attention",
    )(place, doc, q, qt, g, gt, own, px, p2, sw)


def queries_kernel(ds_ref, own_ref, px_ref, p2_ref, sw_ref, out_ref, kv_ref):
    for slot, ref in enumerate((own_ref, px_ref, p2_ref, sw_ref)):
        kv_ref[:, slot * TOK : (slot + 1) * TOK] = ref[...]
    for head in range(HEADS):
        rows = slice(head * TOK, (head + 1) * TOK)
        total = lax.dot_general(
            kv_ref[...], ds_ref[rows, :], (((1,), (1,)), ((), ())), preferred_element_type=jnp.float32
        )
        out_ref[head] = (total * softmax_scale).astype(jnp.bfloat16)


def query_grads(ds, own, px, p2, sw):
    return pl.pallas_call(
        queries_kernel,
        out_shape=jax.ShapeDtypeStruct((HEADS, KVW, TOK), jnp.bfloat16),
        in_specs=[whole] * 5,
        out_specs=whole,
        scratch_shapes=[pltpu.VMEM((KVW, 4 * TOK), jnp.bfloat16)],
        cost_estimate=pl.CostEstimate(
            flops=2 * ROWS * 4 * TOK * KVW, bytes_accessed=2 << 20, transcendentals=0
        ),
        compiler_params=pltpu.CompilerParams(vmem_limit_bytes=12 << 20),
        name="query_grads",
    )(ds, own, px, p2, sw)


def small_call(kernel, name, out_shape, count, scratch=()):
    outs = out_shape if isinstance(out_shape, tuple) else (out_shape,)
    specs = (whole,) * len(outs)
    return pl.pallas_call(
        kernel,
        out_shape=out_shape,
        in_specs=[scalars] + [whole] * count,
        out_specs=specs if isinstance(out_shape, tuple) else whole,
        scratch_shapes=list(scratch),
        cost_estimate=pl.CostEstimate(flops=1 << 19, bytes_accessed=1 << 20, transcendentals=0),
        compiler_params=pltpu.CompilerParams(vmem_limit_bytes=8 << 20),
        name=name,
    )


def join_kernel(place, keep_ref, came_ref, next_ref, over_ref):
    odd = lax.rem(place[0], 2) == 1
    for part in range(KVW // PART):
        cols = slice(part * PART, (part + 1) * PART)
        side = came_ref[1, cols, :].astype(jnp.float32)
        next_ref[cols, :] = (keep_ref[1, cols, :] + side).astype(jnp.bfloat16)
        far = came_ref[0, cols, :].astype(jnp.float32)
        over_ref[cols, :] = jnp.where(odd, far, jnp.zeros_like(far)).astype(jnp.bfloat16)


def total_kernel(place, keep_ref, came_ref, next_ref, over_ref, out_ref, sum_ref):
    even = lax.rem(place[0], 2) == 0
    for part in range(KVW // PART):
        cols = slice(part * PART, (part + 1) * PART)
        near = came_ref[0, cols, :].astype(jnp.float32)
        total = keep_ref[0, cols, :] + jnp.where(even, near, jnp.zeros_like(near))
        total = total + next_ref[cols, :].astype(jnp.float32)
        sum_ref[cols, :] = total + over_ref[cols, :].astype(jnp.float32)
    for share in range(SHARES):
        rows = slice(SHARE * share, SHARE * (share + 1))
        out_ref[share] = sum_ref[rows, :].astype(jnp.bfloat16)


def reduce_kernel(place, came_ref, out_ref):
    total = came_ref[0].astype(jnp.float32)
    for source in range(1, SHARES):
        total = total + came_ref[source].astype(jnp.float32)
    total = total.astype(jnp.bfloat16)
    for share in range(SHARES):
        out_ref[share] = total


def finish_kernel(place, came_ref, out_ref):
    for share in range(SHARES):
        rows = slice(SHARE * share, SHARE * (share + 1))
        out_ref[rows, :] = came_ref[share].astype(jnp.float32)


def routes(count):
    across = SHARES // 2

    def pairs(moves):
        return [
            (a * SHARES + head, b * SHARES + (head ^ other))
            for a, b, other in moves
            if 0 <= b < count
            for head in range(SHARES)
        ]

    halo = pairs([(i, i + 2, across) for i in range(count)])
    mixed = pairs([(i, i + 1 + 2 * (i % 2), 0) for i in range(count)])
    back = pairs([(i, i - 2, across) for i in range(count)])
    over = pairs([(i, i - 4, 0) for i in range(1, count, 2)])
    return halo, mixed, back, over


def per_device(queries, latent_kv, grad_out, doc_start):
    tokens, _, width = queries.shape
    everyone = SEQ + HEAD
    swap = [(0, 1), (1, 0)]
    halo, mixed, back, over = routes(lax.axis_size(SEQ))
    place = lax.axis_index(SEQ).astype(jnp.int32).reshape(1)

    own = latent_kv.T
    p2 = lax.ppermute(own, everyone, halo)
    px = lax.ppermute(own, everyone, mixed)
    sw = lax.ppermute(p2, "core", swap)

    q = queries.transpose(1, 0, 2).reshape(ROWS, width)
    qt = queries.transpose(2, 1, 0).reshape(width, ROWS)
    g = grad_out.transpose(1, 0, 2).reshape(ROWS, LAT)
    gt = jnp.pad(grad_out.transpose(2, 1, 0).reshape(LAT, ROWS), ((0, width - LAT), (0, 0)))
    doc = doc_start.astype(jnp.float32).reshape(1, tokens)

    keep, send, ds = attention(place, doc, q, qt, g, gt, own, px, p2, sw)
    came = lax.ppermute(send, "core", swap)
    block = jax.ShapeDtypeStruct((width, tokens), jnp.bfloat16)
    pieces = jax.ShapeDtypeStruct((SHARES, SHARE, tokens), jnp.bfloat16)
    to_next, to_over = small_call(join_kernel, "join", (block, block), 2)(place, keep, came)
    ds, to_next, to_over = lax.optimization_barrier((ds, to_next, to_over))
    to_next = lax.ppermute(to_next, everyone, back)
    to_over = lax.ppermute(to_over, everyone, over)
    query_grad = query_grads(ds, own, px, p2, sw)
    to_next, to_over, query_grad = lax.optimization_barrier((to_next, to_over, query_grad))

    terms = small_call(
        total_kernel, "total", pieces, 4, [pltpu.VMEM((width, tokens), jnp.float32)]
    )(place, keep, came, to_next, to_over)
    terms = lax.all_to_all(terms, HEAD, 0, 0, tiled=True)
    terms = small_call(reduce_kernel, "reduce", pieces, 1)(place, terms)
    grad = lax.all_to_all(terms, HEAD, 0, 0, tiled=True)
    out = jax.ShapeDtypeStruct((width, tokens), jnp.float32)
    grad = small_call(finish_kernel, "finish", out, 1)(place, grad)
    return query_grad.transpose(2, 0, 1), grad.T


def solution(mesh):
    fine = Mesh(mesh.devices.reshape(8, 2, 2, 4, 8), ("z", "xh", "core", "xl", "y"))
    in_specs = (P(SEQ, HEAD, None), P(SEQ, None), P(SEQ, HEAD, None), P(SEQ))
    out_specs = (P(SEQ, HEAD, None), P(SEQ, None))
    return jax.shard_map(
        per_device, mesh=fine, in_specs=in_specs, out_specs=out_specs, check_vma=False
    )
```

```python
import jax
import jax.numpy as jnp
from jax import lax
from jax.experimental import pallas as pl
from jax.experimental.pallas import tpu as pltpu
from jax.sharding import Mesh
from jax.sharding import PartitionSpec as P

LAT = 512
KVW = 576
TOK = 128
HEADS = 4
ROWS = TOK * HEADS
PART = 72
SHARES = 32
SEQ = ("z", "xh", "core")
HEAD = ("xl", "y")

softmax_scale = 192.0 ** (-0.5)
lowest = -1e30
whole = pl.BlockSpec(memory_space=pltpu.VMEM)
scalars = pl.BlockSpec(memory_space=pltpu.SMEM)


def f32_dot(a, b):
    return jnp.dot(a, b, preferred_element_type=jnp.float32)


def attention_kernel(
    place, doc_ref, q_ref, qt_ref, g_ref, gt_ref, own_ref, px_ref, p2_ref, sw_ref,
    keep_ref, send_ref, ds_ref, kv_ref, bias_ref, p_ref,
):
    seq = place[0]
    core = lax.rem(seq, 2)
    for slot, ref in enumerate((own_ref, px_ref, p2_ref, sw_ref)):
        kv_ref[:, slot * TOK : (slot + 1) * TOK] = ref[...]
    first = jnp.broadcast_to(doc_ref[...], (TOK, TOK)).T
    row = lax.broadcasted_iota(jnp.int32, (TOK, TOK), 0)
    lane = lax.broadcasted_iota(jnp.int32, (TOK, TOK), 1)
    for slot, back in enumerate((0, 3 - 2 * core, 2, 1 + 2 * core)):
        key = lane + (seq - back) * TOK
        seen = (key <= row + seq * TOK) & (key.astype(jnp.float32) >= first)
        bias_ref[:, slot * TOK : (slot + 1) * TOK] = jnp.where(seen, 0.0, lowest)
    for head in range(HEADS):
        rows = slice(head * TOK, (head + 1) * TOK)
        scores = f32_dot(q_ref[rows, :], kv_ref[...]) * softmax_scale + bias_ref[...]
        grad_probs = f32_dot(g_ref[rows, :], kv_ref[:LAT, :])
        top = jnp.max(scores, axis=1, keepdims=True)
        exps = jnp.exp(scores - top)
        inverse = 1.0 / jnp.sum(exps, axis=1, keepdims=True)
        delta = jnp.sum(exps * grad_probs, axis=1, keepdims=True) * inverse
        probs = exps * inverse
        p_ref[rows, :] = probs.astype(jnp.bfloat16)
        ds_ref[rows, :] = (probs * (grad_probs - delta)).astype(jnp.bfloat16)
    for part in range(KVW // PART):
        cols = slice(part * PART, (part + 1) * PART)
        term = f32_dot(qt_ref[cols, :], ds_ref[...]) * softmax_scale
        term = term + f32_dot(gt_ref[cols, :], p_ref[...])
        keep_ref[0, cols, :] = term[:, 0 * TOK : 1 * TOK]
        send_ref[0, cols, :] = term[:, 1 * TOK : 2 * TOK].astype(jnp.bfloat16)
        keep_ref[1, cols, :] = term[:, 2 * TOK : 3 * TOK]
        send_ref[1, cols, :] = term[:, 3 * TOK : 4 * TOK].astype(jnp.bfloat16)


def attention(place, doc, q, qt, g, gt, own, px, p2, sw):
    return pl.pallas_call(
        attention_kernel,
        out_shape=(
            jax.ShapeDtypeStruct((2, KVW, TOK), jnp.float32),
            jax.ShapeDtypeStruct((2, KVW, TOK), jnp.bfloat16),
            jax.ShapeDtypeStruct((ROWS, 4 * TOK), jnp.bfloat16),
        ),
        in_specs=[scalars] + [whole] * 9,
        out_specs=(whole, whole, whole),
        scratch_shapes=[
            pltpu.VMEM((KVW, 4 * TOK), jnp.bfloat16),
            pltpu.VMEM((TOK, 4 * TOK), jnp.float32),
            pltpu.VMEM((ROWS, 4 * TOK), jnp.bfloat16),
        ],
        cost_estimate=pl.CostEstimate(
            flops=4 * 2 * ROWS * 4 * TOK * KVW, bytes_accessed=6 << 20, transcendentals=ROWS * 4 * TOK
        ),
        compiler_params=pltpu.CompilerParams(vmem_limit_bytes=24 << 20),
        name="attention",
    )(place, doc, q, qt, g, gt, own, px, p2, sw)


def queries_kernel(ds_ref, own_ref, px_ref, p2_ref, sw_ref, out_ref, kv_ref):
    for slot, ref in enumerate((own_ref, px_ref, p2_ref, sw_ref)):
        kv_ref[:, slot * TOK : (slot + 1) * TOK] = ref[...]
    for head in range(HEADS):
        rows = slice(head * TOK, (head + 1) * TOK)
        total = lax.dot_general(
            kv_ref[...], ds_ref[rows, :], (((1,), (1,)), ((), ())), preferred_element_type=jnp.float32
        )
        out_ref[head] = (total * softmax_scale).astype(jnp.bfloat16)


def query_grads(ds, own, px, p2, sw):
    return pl.pallas_call(
        queries_kernel,
        out_shape=jax.ShapeDtypeStruct((HEADS, KVW, TOK), jnp.bfloat16),
        in_specs=[whole] * 5,
        out_specs=whole,
        scratch_shapes=[pltpu.VMEM((KVW, 4 * TOK), jnp.bfloat16)],
        cost_estimate=pl.CostEstimate(
            flops=2 * ROWS * 4 * TOK * KVW, bytes_accessed=2 << 20, transcendentals=0
        ),
        compiler_params=pltpu.CompilerParams(vmem_limit_bytes=12 << 20),
        name="query_grads",
    )(ds, own, px, p2, sw)


def small_call(kernel, name, out_shape, count):
    outs = out_shape if isinstance(out_shape, tuple) else (out_shape,)
    specs = (whole,) * len(outs)
    return pl.pallas_call(
        kernel,
        out_shape=out_shape,
        in_specs=[scalars] + [whole] * count,
        out_specs=specs if isinstance(out_shape, tuple) else whole,
        cost_estimate=pl.CostEstimate(flops=1 << 19, bytes_accessed=1 << 20, transcendentals=0),
        compiler_params=pltpu.CompilerParams(vmem_limit_bytes=8 << 20),
        name=name,
    )


def join_kernel(place, keep_ref, came_ref, next_ref, over_ref):
    odd = lax.rem(place[0], 2) == 1
    for part in range(KVW // PART):
        cols = slice(part * PART, (part + 1) * PART)
        side = came_ref[1, cols, :].astype(jnp.float32)
        next_ref[cols, :] = (keep_ref[1, cols, :] + side).astype(jnp.bfloat16)
        far = came_ref[0, cols, :].astype(jnp.float32)
        over_ref[cols, :] = jnp.where(odd, far, jnp.zeros_like(far)).astype(jnp.bfloat16)


def total_kernel(place, keep_ref, came_ref, next_ref, over_ref, out_ref):
    even = lax.rem(place[0], 2) == 0
    for part in range(KVW // PART):
        cols = slice(part * PART, (part + 1) * PART)
        near = came_ref[0, cols, :].astype(jnp.float32)
        total = keep_ref[0, cols, :] + jnp.where(even, near, jnp.zeros_like(near))
        total = total + next_ref[cols, :].astype(jnp.float32)
        out_ref[part] = (total + over_ref[cols, :].astype(jnp.float32)).astype(jnp.bfloat16)


def reduce_kernel(place, came_ref, out_ref):
    total = came_ref[0].astype(jnp.float32)
    for source in range(1, came_ref.shape[0]):
        total = total + came_ref[source].astype(jnp.float32)
    total = total.astype(jnp.bfloat16)
    for copy in range(out_ref.shape[0]):
        out_ref[copy] = total


def finish_kernel(place, came_ref, out_ref):
    for part in range(KVW // PART):
        out_ref[slice(part * PART, (part + 1) * PART), :] = came_ref[part].astype(jnp.float32)


def routes(count):
    across = SHARES // 2

    def pairs(moves):
        return [
            (a * SHARES + head, b * SHARES + (head ^ other))
            for a, b, other in moves
            if 0 <= b < count
            for head in range(SHARES)
        ]

    halo = pairs([(i, i + 2, across) for i in range(count)])
    mixed = pairs([(i, i + 1 + 2 * (i % 2), 0) for i in range(count)])
    back = pairs([(i, i - 2, across) for i in range(count)])
    over = pairs([(i, i - 4, 0) for i in range(1, count, 2)])
    return halo, mixed, back, over


def per_device(queries, latent_kv, grad_out, doc_start):
    tokens, _, width = queries.shape
    everyone = SEQ + HEAD
    swap = [(0, 1), (1, 0)]
    halo, mixed, back, over = routes(lax.axis_size(SEQ))
    place = lax.axis_index(SEQ).astype(jnp.int32).reshape(1)

    own = latent_kv.T
    p2 = lax.ppermute(own, everyone, halo)
    q = queries.transpose(1, 0, 2).reshape(ROWS, width)
    qt = queries.transpose(2, 1, 0).reshape(width, ROWS)
    g = grad_out.transpose(1, 0, 2).reshape(ROWS, LAT)
    gt = jnp.pad(grad_out.transpose(2, 1, 0).reshape(LAT, ROWS), ((0, width - LAT), (0, 0)))
    doc = doc_start.astype(jnp.float32).reshape(1, tokens)
    after, q, qt, g, gt, doc = lax.optimization_barrier((own, q, qt, g, gt, doc))
    px = lax.ppermute(after, everyone, mixed)
    sw = lax.ppermute(p2, "core", swap)

    keep, send, ds = attention(place, doc, q, qt, g, gt, own, px, p2, sw)
    came = lax.ppermute(send, "core", swap)
    block = jax.ShapeDtypeStruct((width, tokens), jnp.bfloat16)
    to_next, to_over = small_call(join_kernel, "join", (block, block), 2)(place, keep, came)
    ds, to_next, to_over = lax.optimization_barrier((ds, to_next, to_over))
    to_next = lax.ppermute(to_next, everyone, back)
    to_over = lax.ppermute(to_over, everyone, over)
    query_grad = query_grads(ds, own, px, p2, sw)
    to_next, to_over, query_grad = lax.optimization_barrier((to_next, to_over, query_grad))

    def pieces(count):
        return jax.ShapeDtypeStruct((count, PART, tokens), jnp.bfloat16)

    rows, lines = lax.axis_size("y"), lax.axis_size("xl")
    terms = small_call(total_kernel, "total", pieces(rows), 4)(place, keep, came, to_next, to_over)
    terms = lax.all_to_all(terms, "y", 0, 0, tiled=True)
    terms = small_call(reduce_kernel, "reduce_rows", pieces(lines), 1)(place, terms)
    terms = lax.all_to_all(terms, "xl", 0, 0, tiled=True)
    terms = small_call(reduce_kernel, "reduce_lines", pieces(rows), 1)(place, terms)
    grad = lax.all_to_all(terms, "y", 0, 0, tiled=True)
    out = jax.ShapeDtypeStruct((width, tokens), jnp.float32)
    grad = small_call(finish_kernel, "finish", out, 1)(place, grad)
    return query_grad.transpose(2, 0, 1), grad.T


def solution(mesh):
    fine = Mesh(mesh.devices.reshape(8, 2, 2, 4, 8), ("z", "xh", "core", "xl", "y"))
    in_specs = (P(SEQ, HEAD, None), P(SEQ, None), P(SEQ, HEAD, None), P(SEQ))
    out_specs = (P(SEQ, HEAD, None), P(SEQ, None))
    return jax.shard_map(
        per_device, mesh=fine, in_specs=in_specs, out_specs=out_specs, check_vma=False
    )
```

```python
import jax
import jax.numpy as jnp
from jax import lax
from jax.experimental import pallas as pl
from jax.experimental.pallas import tpu as pltpu
from jax.sharding import Mesh
from jax.sharding import PartitionSpec as P

LAT = 512
KVW = 576
TOK = 128
HEADS = 4
ROWS = TOK * HEADS
PART = 72
SHARES = 32
WIDE = KVW // (2 * SHARES)
SEQ = ("z", "xh", "core")
HEAD = ("xl", "y")

softmax_scale = 192.0 ** (-0.5)
lowest = -1e30
whole = pl.BlockSpec(memory_space=pltpu.VMEM)
scalars = pl.BlockSpec(memory_space=pltpu.SMEM)


def f32_dot(a, b):
    return jnp.dot(a, b, preferred_element_type=jnp.float32)


def attention_kernel(
    place, doc_ref, q_ref, qt_ref, g_ref, gt_ref, own_ref, px_ref, p2_ref, sw_ref,
    keep_ref, send_ref, ds_ref, kv_ref, bias_ref, p_ref,
):
    seq = place[0]
    core = lax.rem(seq, 2)
    for slot, ref in enumerate((own_ref, px_ref, p2_ref, sw_ref)):
        kv_ref[:, slot * TOK : (slot + 1) * TOK] = ref[...]
    first = jnp.broadcast_to(doc_ref[...], (TOK, TOK)).T
    row = lax.broadcasted_iota(jnp.int32, (TOK, TOK), 0)
    lane = lax.broadcasted_iota(jnp.int32, (TOK, TOK), 1)
    for slot, back in enumerate((0, 3 - 2 * core, 2, 1 + 2 * core)):
        key = lane + (seq - back) * TOK
        seen = (key <= row + seq * TOK) & (key.astype(jnp.float32) >= first)
        bias_ref[:, slot * TOK : (slot + 1) * TOK] = jnp.where(seen, 0.0, lowest)
    for head in range(HEADS):
        rows = slice(head * TOK, (head + 1) * TOK)
        scores = f32_dot(q_ref[rows, :], kv_ref[...]) * softmax_scale + bias_ref[...]
        grad_probs = f32_dot(g_ref[rows, :], kv_ref[:LAT, :])
        top = jnp.max(scores, axis=1, keepdims=True)
        exps = jnp.exp(scores - top)
        inverse = 1.0 / jnp.sum(exps, axis=1, keepdims=True)
        delta = jnp.sum(exps * grad_probs, axis=1, keepdims=True) * inverse
        probs = exps * inverse
        p_ref[rows, :] = probs.astype(jnp.bfloat16)
        ds_ref[rows, :] = (probs * (grad_probs - delta)).astype(jnp.bfloat16)
    for part in range(KVW // PART):
        cols = slice(part * PART, (part + 1) * PART)
        term = f32_dot(qt_ref[cols, :], ds_ref[...]) * softmax_scale
        term = term + f32_dot(gt_ref[cols, :], p_ref[...])
        keep_ref[0, cols, :] = term[:, 0 * TOK : 1 * TOK]
        send_ref[0, cols, :] = term[:, 1 * TOK : 2 * TOK].astype(jnp.bfloat16)
        keep_ref[1, cols, :] = term[:, 2 * TOK : 3 * TOK]
        send_ref[1, cols, :] = term[:, 3 * TOK : 4 * TOK].astype(jnp.bfloat16)


def attention(place, doc, q, qt, g, gt, own, px, p2, sw):
    return pl.pallas_call(
        attention_kernel,
        out_shape=(
            jax.ShapeDtypeStruct((2, KVW, TOK), jnp.float32),
            jax.ShapeDtypeStruct((2, KVW, TOK), jnp.bfloat16),
            jax.ShapeDtypeStruct((ROWS, 4 * TOK), jnp.bfloat16),
        ),
        in_specs=[scalars] + [whole] * 9,
        out_specs=(whole, whole, whole),
        scratch_shapes=[
            pltpu.VMEM((KVW, 4 * TOK), jnp.bfloat16),
            pltpu.VMEM((TOK, 4 * TOK), jnp.float32),
            pltpu.VMEM((ROWS, 4 * TOK), jnp.bfloat16),
        ],
        cost_estimate=pl.CostEstimate(
            flops=4 * 2 * ROWS * 4 * TOK * KVW, bytes_accessed=6 << 20, transcendentals=ROWS * 4 * TOK
        ),
        compiler_params=pltpu.CompilerParams(vmem_limit_bytes=24 << 20),
        name="attention",
    )(place, doc, q, qt, g, gt, own, px, p2, sw)


def queries_kernel(ds_ref, own_ref, px_ref, p2_ref, sw_ref, out_ref, kv_ref):
    for slot, ref in enumerate((own_ref, px_ref, p2_ref, sw_ref)):
        kv_ref[:, slot * TOK : (slot + 1) * TOK] = ref[...]
    for head in range(HEADS):
        rows = slice(head * TOK, (head + 1) * TOK)
        total = lax.dot_general(
            kv_ref[...], ds_ref[rows, :], (((1,), (1,)), ((), ())), preferred_element_type=jnp.float32
        )
        out_ref[head] = (total * softmax_scale).astype(jnp.bfloat16)


def query_grads(ds, own, px, p2, sw):
    return pl.pallas_call(
        queries_kernel,
        out_shape=jax.ShapeDtypeStruct((HEADS, KVW, TOK), jnp.bfloat16),
        in_specs=[whole] * 5,
        out_specs=whole,
        scratch_shapes=[pltpu.VMEM((KVW, 4 * TOK), jnp.bfloat16)],
        cost_estimate=pl.CostEstimate(
            flops=2 * ROWS * 4 * TOK * KVW, bytes_accessed=2 << 20, transcendentals=0
        ),
        compiler_params=pltpu.CompilerParams(vmem_limit_bytes=12 << 20),
        name="query_grads",
    )(ds, own, px, p2, sw)


def small_call(kernel, name, out_shape, count, scratch=()):
    outs = out_shape if isinstance(out_shape, tuple) else (out_shape,)
    specs = (whole,) * len(outs)
    return pl.pallas_call(
        kernel,
        out_shape=out_shape,
        in_specs=[scalars] + [whole] * count,
        out_specs=specs if isinstance(out_shape, tuple) else whole,
        scratch_shapes=list(scratch),
        cost_estimate=pl.CostEstimate(flops=1 << 19, bytes_accessed=1 << 20, transcendentals=0),
        compiler_params=pltpu.CompilerParams(vmem_limit_bytes=8 << 20),
        name=name,
    )


def join_kernel(place, keep_ref, came_ref, next_ref, over_ref):
    odd = lax.rem(place[0], 2) == 1
    for part in range(KVW // PART):
        cols = slice(part * PART, (part + 1) * PART)
        side = came_ref[1, cols, :].astype(jnp.float32)
        next_ref[cols, :] = (keep_ref[1, cols, :] + side).astype(jnp.bfloat16)
        far = came_ref[0, cols, :].astype(jnp.float32)
        over_ref[cols, :] = jnp.where(odd, far, jnp.zeros_like(far)).astype(jnp.bfloat16)


def total_kernel(place, keep_ref, came_ref, next_ref, over_ref, out_ref, sum_ref):
    even = lax.rem(place[0], 2) == 0
    for part in range(KVW // PART):
        cols = slice(part * PART, (part + 1) * PART)
        near = came_ref[0, cols, :].astype(jnp.float32)
        total = keep_ref[0, cols, :] + jnp.where(even, near, jnp.zeros_like(near))
        total = total + next_ref[cols, :].astype(jnp.float32)
        sum_ref[cols, :] = total + over_ref[cols, :].astype(jnp.float32)
    for lanes in range(WIDE):
        cols = slice(lanes * TOK, (lanes + 1) * TOK)
        picked = sum_ref[pl.ds(lanes, 2 * SHARES, stride=WIDE), :]
        out_ref[:, cols] = picked.astype(jnp.bfloat16)


def reduce_kernel(place, came_ref, out_ref):
    total = came_ref[0].astype(jnp.float32)
    for source in range(1, SHARES):
        total = total + came_ref[source].astype(jnp.float32)
    total = total.astype(jnp.bfloat16)
    for share in range(SHARES):
        out_ref[share] = total


def finish_kernel(place, came_ref, out_ref):
    for lanes in range(WIDE):
        cols = slice(lanes * TOK, (lanes + 1) * TOK)
        out_ref[pl.ds(lanes, 2 * SHARES, stride=WIDE), :] = came_ref[:, cols].astype(jnp.float32)


def routes(count):
    across = SHARES // 2

    def pairs(moves):
        return [
            (a * SHARES + head, b * SHARES + (head ^ other))
            for a, b, other in moves
            if 0 <= b < count
            for head in range(SHARES)
        ]

    halo = pairs([(i, i + 2, across) for i in range(count)])
    mixed = pairs([(i, i + 1 + 2 * (i % 2), 0) for i in range(count)])
    back = pairs([(i, i - 2, across) for i in range(count)])
    over = pairs([(i, i - 4, 0) for i in range(1, count, 2)])
    return halo, mixed, back, over


def per_device(queries, latent_kv, grad_out, doc_start):
    tokens, _, width = queries.shape
    everyone = SEQ + HEAD
    swap = [(0, 1), (1, 0)]
    halo, mixed, back, over = routes(lax.axis_size(SEQ))
    place = lax.axis_index(SEQ).astype(jnp.int32).reshape(1)

    own = latent_kv.T
    p2 = lax.ppermute(own, everyone, halo)
    px = lax.ppermute(own, everyone, mixed)
    sw = lax.ppermute(p2, "core", swap)

    q = queries.transpose(1, 0, 2).reshape(ROWS, width)
    qt = queries.transpose(2, 1, 0).reshape(width, ROWS)
    g = grad_out.transpose(1, 0, 2).reshape(ROWS, LAT)
    gt = jnp.pad(grad_out.transpose(2, 1, 0).reshape(LAT, ROWS), ((0, width - LAT), (0, 0)))
    doc = doc_start.astype(jnp.float32).reshape(1, tokens)

    keep, send, ds = attention(place, doc, q, qt, g, gt, own, px, p2, sw)
    came = lax.ppermute(send, "core", swap)
    block = jax.ShapeDtypeStruct((width, tokens), jnp.bfloat16)
    flat = jax.ShapeDtypeStruct((2 * SHARES, WIDE * tokens), jnp.bfloat16)
    pieces = jax.ShapeDtypeStruct((SHARES, 2, WIDE * tokens), jnp.bfloat16)
    to_next, to_over = small_call(join_kernel, "join", (block, block), 2)(place, keep, came)
    ds, to_next, to_over = lax.optimization_barrier((ds, to_next, to_over))
    to_next = lax.ppermute(to_next, everyone, back)
    to_over = lax.ppermute(to_over, everyone, over)
    query_grad = query_grads(ds, own, px, p2, sw)
    to_next, to_over, query_grad = lax.optimization_barrier((to_next, to_over, query_grad))

    terms = small_call(
        total_kernel, "total", flat, 4, [pltpu.VMEM((width, tokens), jnp.float32)]
    )(place, keep, came, to_next, to_over)
    terms = lax.all_to_all(terms.reshape(pieces.shape), HEAD, 0, 0, tiled=True)
    terms = small_call(reduce_kernel, "reduce", pieces, 1)(place, terms)
    grad = lax.all_to_all(terms, HEAD, 0, 0, tiled=True)
    out = jax.ShapeDtypeStruct((width, tokens), jnp.float32)
    grad = small_call(finish_kernel, "finish", out, 1)(place, grad.reshape(flat.shape))
    return query_grad.transpose(2, 0, 1), grad.T


def solution(mesh):
    fine = Mesh(mesh.devices.reshape(8, 2, 2, 4, 8), ("z", "xh", "core", "xl", "y"))
    in_specs = (P(SEQ, HEAD, None), P(SEQ, None), P(SEQ, HEAD, None), P(SEQ))
    out_specs = (P(SEQ, HEAD, None), P(SEQ, None))
    return jax.shard_map(
        per_device, mesh=fine, in_specs=in_specs, out_specs=out_specs, check_vma=False
    )
```

```python
import jax
import jax.numpy as jnp
from jax import lax
from jax.experimental import pallas as pl
from jax.experimental.pallas import tpu as pltpu
from jax.sharding import Mesh
from jax.sharding import PartitionSpec as P

LAT = 512
KVW = 576
TOK = 128
HEADS = 4
ROWS = TOK * HEADS
PART = 72
SHARES = 32
WIDE = KVW // (2 * SHARES)
SEQ = ("z", "xh", "core")
HEAD = ("xl", "y")

softmax_scale = 192.0 ** (-0.5)
lowest = -1e30
whole = pl.BlockSpec(memory_space=pltpu.VMEM)
scalars = pl.BlockSpec(memory_space=pltpu.SMEM)


def f32_dot(a, b):
    return jnp.dot(a, b, preferred_element_type=jnp.float32)


def load_pair(place, doc_ref, backs, blocks, kv_ref, bias_ref):
    seq = place[0]
    first = jnp.broadcast_to(doc_ref[...], (TOK, TOK)).T
    row = lax.broadcasted_iota(jnp.int32, (TOK, TOK), 0)
    lane = lax.broadcasted_iota(jnp.int32, (TOK, TOK), 1)
    for slot, (back, ref) in enumerate(zip(backs, blocks)):
        cols = slice(slot * TOK, (slot + 1) * TOK)
        kv_ref[:, cols] = ref[...]
        key = lane + (seq - back) * TOK
        seen = (key <= row + seq * TOK) & (key.astype(jnp.float32) >= first)
        bias_ref[:, cols] = jnp.where(seen, 0.0, lowest)


def near_kernel(
    place, doc_ref, q_ref, g_ref, own_ref, px_ref, score_ref, grad_ref, kv_ref, bias_ref
):
    core = lax.rem(place[0], 2)
    load_pair(place, doc_ref, (0, 3 - 2 * core), (own_ref, px_ref), kv_ref, bias_ref)
    for head in range(HEADS):
        rows = slice(head * TOK, (head + 1) * TOK)
        score_ref[rows, :] = f32_dot(q_ref[rows, :], kv_ref[...]) * softmax_scale + bias_ref[...]
        grad_ref[rows, :] = f32_dot(g_ref[rows, :], kv_ref[:LAT, :])


def add_terms(qt_ref, gt_ref, ds_ref, p_ref, part, lanes):
    cols = slice(part * PART, (part + 1) * PART)
    term = f32_dot(qt_ref[cols, :], ds_ref[:, lanes]) * softmax_scale
    return cols, term + f32_dot(gt_ref[cols, :], p_ref[:, lanes])


def attention_kernel(
    place, doc_ref, q_ref, qt_ref, g_ref, gt_ref, score_ref, grad_ref, p2_ref, sw_ref,
    send_ref, p_ref, ds_ref, kv_ref, bias_ref,
):
    core = lax.rem(place[0], 2)
    load_pair(place, doc_ref, (2, 1 + 2 * core), (p2_ref, sw_ref), kv_ref, bias_ref)
    for head in range(HEADS):
        rows = slice(head * TOK, (head + 1) * TOK)
        far = f32_dot(q_ref[rows, :], kv_ref[...]) * softmax_scale + bias_ref[...]
        far_grads = f32_dot(g_ref[rows, :], kv_ref[:LAT, :])
        near, near_grads = score_ref[rows, :], grad_ref[rows, :]
        top = jnp.max(jnp.maximum(near, far), axis=1, keepdims=True)
        near, far = jnp.exp(near - top), jnp.exp(far - top)
        inverse = 1.0 / jnp.sum(near + far, axis=1, keepdims=True)
        delta = jnp.sum(near * near_grads + far * far_grads, axis=1, keepdims=True) * inverse
        for half, (exps, grads) in enumerate(((near, near_grads), (far, far_grads))):
            probs = exps * inverse
            for slot in range(2):
                mine = slice(slot * TOK, (slot + 1) * TOK)
                place_at = half + (0 if slot == 1 else 2)
                lanes = slice(place_at * TOK, (place_at + 1) * TOK)
                p_ref[rows, lanes] = probs[:, mine].astype(jnp.bfloat16)
                ds_ref[rows, lanes] = (probs[:, mine] * (grads[:, mine] - delta)).astype(
                    jnp.bfloat16
                )
    for part in range(KVW // PART):
        cols, term = add_terms(qt_ref, gt_ref, ds_ref, p_ref, part, slice(0, 2 * TOK))
        send_ref[0, cols, :] = term[:, :TOK].astype(jnp.bfloat16)
        send_ref[1, cols, :] = term[:, TOK:].astype(jnp.bfloat16)


def keep_kernel(place, qt_ref, gt_ref, p_ref, ds_ref, keep_ref):
    for part in range(KVW // PART):
        cols, term = add_terms(qt_ref, gt_ref, ds_ref, p_ref, part, slice(2 * TOK, 4 * TOK))
        keep_ref[0, cols, :] = term[:, :TOK]
        keep_ref[1, cols, :] = term[:, TOK:]


def queries_kernel(ds_ref, own_ref, px_ref, p2_ref, sw_ref, out_ref, kv_ref):
    for slot, ref in enumerate((px_ref, sw_ref, own_ref, p2_ref)):
        kv_ref[:, slot * TOK : (slot + 1) * TOK] = ref[...]
    for head in range(HEADS):
        rows = slice(head * TOK, (head + 1) * TOK)
        total = lax.dot_general(
            kv_ref[...], ds_ref[rows, :], (((1,), (1,)), ((), ())), preferred_element_type=jnp.float32
        )
        out_ref[head] = (total * softmax_scale).astype(jnp.bfloat16)


def query_grads(ds, own, px, p2, sw):
    return pl.pallas_call(
        queries_kernel,
        out_shape=jax.ShapeDtypeStruct((HEADS, KVW, TOK), jnp.bfloat16),
        in_specs=[whole] * 5,
        out_specs=whole,
        scratch_shapes=[pltpu.VMEM((KVW, 4 * TOK), jnp.bfloat16)],
        cost_estimate=pl.CostEstimate(
            flops=2 * ROWS * 4 * TOK * KVW, bytes_accessed=2 << 20, transcendentals=0
        ),
        compiler_params=pltpu.CompilerParams(vmem_limit_bytes=12 << 20),
        name="query_grads",
    )(ds, own, px, p2, sw)


def call(kernel, name, out_shape, count, scratch=(), macs=1 << 18, limit=8):
    outs = out_shape if isinstance(out_shape, tuple) else (out_shape,)
    specs = (whole,) * len(outs)
    return pl.pallas_call(
        kernel,
        out_shape=out_shape,
        in_specs=[scalars] + [whole] * count,
        out_specs=specs if isinstance(out_shape, tuple) else whole,
        scratch_shapes=list(scratch),
        cost_estimate=pl.CostEstimate(flops=2 * macs, bytes_accessed=1 << 20, transcendentals=0),
        compiler_params=pltpu.CompilerParams(vmem_limit_bytes=limit << 20),
        name=name,
    )


def join_kernel(place, keep_ref, came_ref, next_ref, over_ref):
    odd = lax.rem(place[0], 2) == 1
    for part in range(KVW // PART):
        cols = slice(part * PART, (part + 1) * PART)
        side = came_ref[1, cols, :].astype(jnp.float32)
        next_ref[cols, :] = (keep_ref[1, cols, :] + side).astype(jnp.bfloat16)
        far = came_ref[0, cols, :].astype(jnp.float32)
        over_ref[cols, :] = jnp.where(odd, far, jnp.zeros_like(far)).astype(jnp.bfloat16)


def total_kernel(place, keep_ref, came_ref, next_ref, over_ref, out_ref, sum_ref):
    even = lax.rem(place[0], 2) == 0
    for part in range(KVW // PART):
        cols = slice(part * PART, (part + 1) * PART)
        near = came_ref[0, cols, :].astype(jnp.float32)
        total = keep_ref[0, cols, :] + jnp.where(even, near, jnp.zeros_like(near))
        total = total + next_ref[cols, :].astype(jnp.float32)
        sum_ref[cols, :] = total + over_ref[cols, :].astype(jnp.float32)
    for lanes in range(WIDE):
        cols = slice(lanes * TOK, (lanes + 1) * TOK)
        picked = sum_ref[pl.ds(lanes, 2 * SHARES, stride=WIDE), :]
        out_ref[:, cols] = picked.astype(jnp.bfloat16)


def reduce_kernel(place, came_ref, out_ref):
    total = came_ref[0].astype(jnp.float32)
    for source in range(1, SHARES):
        total = total + came_ref[source].astype(jnp.float32)
    total = total.astype(jnp.bfloat16)
    for share in range(SHARES):
        out_ref[share] = total


def finish_kernel(place, came_ref, out_ref):
    for lanes in range(WIDE):
        cols = slice(lanes * TOK, (lanes + 1) * TOK)
        out_ref[pl.ds(lanes, 2 * SHARES, stride=WIDE), :] = came_ref[:, cols].astype(jnp.float32)


def routes(count):
    across = SHARES // 2

    def pairs(moves):
        return [
            (a * SHARES + head, b * SHARES + (head ^ other))
            for a, b, other in moves
            if 0 <= b < count
            for head in range(SHARES)
        ]

    halo = pairs([(i, i + 2, across) for i in range(count)])
    mixed = pairs([(i, i + 1 + 2 * (i % 2), 0) for i in range(count)])
    back = pairs([(i, i - 2, across) for i in range(count)])
    over = pairs([(i, i - 4, 0) for i in range(1, count, 2)])
    return halo, mixed, back, over


def per_device(queries, latent_kv, grad_out, doc_start):
    tokens, _, width = queries.shape
    everyone = SEQ + HEAD
    swap = [(0, 1), (1, 0)]
    halo, mixed, back, over = routes(lax.axis_size(SEQ))
    place = lax.axis_index(SEQ).astype(jnp.int32).reshape(1)

    own = latent_kv.T
    p2 = lax.ppermute(own, everyone, halo)
    px = lax.ppermute(own, everyone, mixed)
    sw = lax.ppermute(p2, "core", swap)

    q = queries.transpose(1, 0, 2).reshape(ROWS, width)
    qt = queries.transpose(2, 1, 0).reshape(width, ROWS)
    g = grad_out.transpose(1, 0, 2).reshape(ROWS, LAT)
    gt = jnp.pad(grad_out.transpose(2, 1, 0).reshape(LAT, ROWS), ((0, width - LAT), (0, 0)))
    doc = doc_start.astype(jnp.float32).reshape(1, tokens)

    pair = [pltpu.VMEM((width, 2 * TOK), jnp.bfloat16), pltpu.VMEM((TOK, 2 * TOK), jnp.float32)]
    half = jax.ShapeDtypeStruct((ROWS, 2 * TOK), jnp.float32)
    table = jax.ShapeDtypeStruct((ROWS, 4 * TOK), jnp.bfloat16)
    sent = jax.ShapeDtypeStruct((2, width, tokens), jnp.bfloat16)
    kept = jax.ShapeDtypeStruct((2, width, tokens), jnp.float32)
    work = 2 * ROWS * TOK * (width + LAT)
    px_now, p2_now = lax.optimization_barrier((px, p2))
    scores, grads = call(near_kernel, "near", (half, half), 5, pair, work, 12)(
        place, doc, q, g, own, px_now
    )
    send, probs, ds = call(attention_kernel, "attention", (sent, table, table), 9, pair, 2 * work, 20)(
        place, doc, q, qt, g, gt, scores, grads, p2_now, sw
    )
    came = lax.ppermute(send, "core", swap)
    keep = call(keep_kernel, "keep", kept, 4, (), work, 12)(place, qt, gt, probs, ds)
    block = jax.ShapeDtypeStruct((width, tokens), jnp.bfloat16)
    flat = jax.ShapeDtypeStruct((2 * SHARES, WIDE * tokens), jnp.bfloat16)
    pieces = jax.ShapeDtypeStruct((SHARES, 2, WIDE * tokens), jnp.bfloat16)
    to_next, to_over = call(join_kernel, "join", (block, block), 2)(place, keep, came)
    ds, to_next, to_over = lax.optimization_barrier((ds, to_next, to_over))
    to_next = lax.ppermute(to_next, everyone, back)
    to_over = lax.ppermute(to_over, everyone, over)
    query_grad = query_grads(ds, own, px, p2, sw)
    to_next, to_over, query_grad = lax.optimization_barrier((to_next, to_over, query_grad))

    terms = call(
        total_kernel, "total", flat, 4, [pltpu.VMEM((width, tokens), jnp.float32)]
    )(place, keep, came, to_next, to_over)
    terms = lax.all_to_all(terms.reshape(pieces.shape), HEAD, 0, 0, tiled=True)
    terms = call(reduce_kernel, "reduce", pieces, 1)(place, terms)
    grad = lax.all_to_all(terms, HEAD, 0, 0, tiled=True)
    out = jax.ShapeDtypeStruct((width, tokens), jnp.float32)
    grad = call(finish_kernel, "finish", out, 1)(place, grad.reshape(flat.shape))
    return query_grad.transpose(2, 0, 1), grad.T


def solution(mesh):
    fine = Mesh(mesh.devices.reshape(8, 2, 2, 4, 8), ("z", "xh", "core", "xl", "y"))
    in_specs = (P(SEQ, HEAD, None), P(SEQ, None), P(SEQ, HEAD, None), P(SEQ))
    out_specs = (P(SEQ, HEAD, None), P(SEQ, None))
    return jax.shard_map(
        per_device, mesh=fine, in_specs=in_specs, out_specs=out_specs, check_vma=False
    )
```

```python
import jax
import jax.numpy as jnp
from jax import lax
from jax.experimental import pallas as pl
from jax.experimental.pallas import tpu as pltpu
from jax.sharding import Mesh
from jax.sharding import PartitionSpec as P

LAT = 512
KVW = 576
TOK = 128
HEADS = 4
ROWS = TOK * HEADS
PART = 72
SHARES = 32
WIDE = KVW // (2 * SHARES)
SEQ = ("z", "xh", "core")
HEAD = ("xl", "y")

softmax_scale = 192.0 ** (-0.5)
lowest = -1e30
whole = pl.BlockSpec(memory_space=pltpu.VMEM)
scalars = pl.BlockSpec(memory_space=pltpu.SMEM)


def f32_dot(a, b):
    return jnp.dot(a, b, preferred_element_type=jnp.float32)


def load_pair(place, doc_ref, backs, blocks, kv_ref, bias_ref):
    seq = place[0]
    first = jnp.broadcast_to(doc_ref[...], (TOK, TOK)).T
    row = lax.broadcasted_iota(jnp.int32, (TOK, TOK), 0)
    lane = lax.broadcasted_iota(jnp.int32, (TOK, TOK), 1)
    for slot, (back, ref) in enumerate(zip(backs, blocks)):
        cols = slice(slot * TOK, (slot + 1) * TOK)
        kv_ref[:, cols] = ref[...]
        key = lane + (seq - back) * TOK
        seen = (key <= row + seq * TOK) & (key.astype(jnp.float32) >= first)
        bias_ref[:, cols] = jnp.where(seen, 0.0, lowest)


def near_kernel(
    place, doc_ref, q_ref, g_ref, px_ref, p2_ref, score_ref, grad_ref, kv_ref, bias_ref
):
    core = lax.rem(place[0], 2)
    load_pair(place, doc_ref, (3 - 2 * core, 2), (px_ref, p2_ref), kv_ref, bias_ref)
    for head in range(HEADS):
        rows = slice(head * TOK, (head + 1) * TOK)
        score_ref[rows, :] = f32_dot(q_ref[rows, :], kv_ref[...]) * softmax_scale + bias_ref[...]
        grad_ref[rows, :] = f32_dot(g_ref[rows, :], kv_ref[:LAT, :])


def add_terms(qt_ref, gt_ref, ds_ref, p_ref, part, lanes):
    cols = slice(part * PART, (part + 1) * PART)
    term = f32_dot(qt_ref[cols, :], ds_ref[:, lanes]) * softmax_scale
    return cols, term + f32_dot(gt_ref[cols, :], p_ref[:, lanes])


def attention_kernel(
    place, doc_ref, q_ref, qt_ref, g_ref, gt_ref, score_ref, grad_ref, own_ref, sw_ref,
    send_ref, p_ref, ds_ref, kv_ref, bias_ref,
):
    core = lax.rem(place[0], 2)
    load_pair(place, doc_ref, (0, 1 + 2 * core), (own_ref, sw_ref), kv_ref, bias_ref)
    for head in range(HEADS):
        rows = slice(head * TOK, (head + 1) * TOK)
        far = f32_dot(q_ref[rows, :], kv_ref[...]) * softmax_scale + bias_ref[...]
        far_grads = f32_dot(g_ref[rows, :], kv_ref[:LAT, :])
        near, near_grads = score_ref[rows, :], grad_ref[rows, :]
        top = jnp.max(jnp.maximum(near, far), axis=1, keepdims=True)
        near, far = jnp.exp(near - top), jnp.exp(far - top)
        inverse = 1.0 / jnp.sum(near + far, axis=1, keepdims=True)
        delta = jnp.sum(near * near_grads + far * far_grads, axis=1, keepdims=True) * inverse
        for half, (exps, grads) in enumerate(((near, near_grads), (far, far_grads))):
            probs = exps * inverse
            for slot in range(2):
                mine = slice(slot * TOK, (slot + 1) * TOK)
                place_at = ((0, 3), (2, 1))[half][slot]
                lanes = slice(place_at * TOK, (place_at + 1) * TOK)
                p_ref[rows, lanes] = probs[:, mine].astype(jnp.bfloat16)
                ds_ref[rows, lanes] = (probs[:, mine] * (grads[:, mine] - delta)).astype(
                    jnp.bfloat16
                )
    for part in range(KVW // PART):
        cols, term = add_terms(qt_ref, gt_ref, ds_ref, p_ref, part, slice(0, 2 * TOK))
        send_ref[0, cols, :] = term[:, :TOK].astype(jnp.bfloat16)
        send_ref[1, cols, :] = term[:, TOK:].astype(jnp.bfloat16)


def keep_kernel(place, qt_ref, gt_ref, p_ref, ds_ref, keep_ref):
    for part in range(KVW // PART):
        cols, term = add_terms(qt_ref, gt_ref, ds_ref, p_ref, part, slice(2 * TOK, 4 * TOK))
        keep_ref[0, cols, :] = term[:, :TOK]
        keep_ref[1, cols, :] = term[:, TOK:]


def queries_kernel(ds_ref, own_ref, px_ref, p2_ref, sw_ref, out_ref, kv_ref):
    for slot, ref in enumerate((px_ref, sw_ref, own_ref, p2_ref)):
        kv_ref[:, slot * TOK : (slot + 1) * TOK] = ref[...]
    for head in range(HEADS):
        rows = slice(head * TOK, (head + 1) * TOK)
        total = lax.dot_general(
            kv_ref[...], ds_ref[rows, :], (((1,), (1,)), ((), ())), preferred_element_type=jnp.float32
        )
        out_ref[head] = (total * softmax_scale).astype(jnp.bfloat16)


def query_grads(ds, own, px, p2, sw):
    return pl.pallas_call(
        queries_kernel,
        out_shape=jax.ShapeDtypeStruct((HEADS, KVW, TOK), jnp.bfloat16),
        in_specs=[whole] * 5,
        out_specs=whole,
        scratch_shapes=[pltpu.VMEM((KVW, 4 * TOK), jnp.bfloat16)],
        cost_estimate=pl.CostEstimate(
            flops=2 * ROWS * 4 * TOK * KVW, bytes_accessed=2 << 20, transcendentals=0
        ),
        compiler_params=pltpu.CompilerParams(vmem_limit_bytes=12 << 20),
        name="query_grads",
    )(ds, own, px, p2, sw)


def call(kernel, name, out_shape, count, scratch=(), macs=1 << 18, limit=8):
    outs = out_shape if isinstance(out_shape, tuple) else (out_shape,)
    specs = (whole,) * len(outs)
    return pl.pallas_call(
        kernel,
        out_shape=out_shape,
        in_specs=[scalars] + [whole] * count,
        out_specs=specs if isinstance(out_shape, tuple) else whole,
        scratch_shapes=list(scratch),
        cost_estimate=pl.CostEstimate(flops=2 * macs, bytes_accessed=1 << 20, transcendentals=0),
        compiler_params=pltpu.CompilerParams(vmem_limit_bytes=limit << 20),
        name=name,
    )


def join_kernel(place, keep_ref, came_ref, next_ref, over_ref):
    odd = lax.rem(place[0], 2) == 1
    for part in range(KVW // PART):
        cols = slice(part * PART, (part + 1) * PART)
        side = came_ref[1, cols, :].astype(jnp.float32)
        next_ref[cols, :] = (keep_ref[1, cols, :] + side).astype(jnp.bfloat16)
        far = came_ref[0, cols, :].astype(jnp.float32)
        over_ref[cols, :] = jnp.where(odd, far, jnp.zeros_like(far)).astype(jnp.bfloat16)


def total_kernel(place, keep_ref, came_ref, next_ref, over_ref, out_ref, sum_ref):
    even = lax.rem(place[0], 2) == 0
    for part in range(KVW // PART):
        cols = slice(part * PART, (part + 1) * PART)
        near = came_ref[0, cols, :].astype(jnp.float32)
        total = keep_ref[0, cols, :] + jnp.where(even, near, jnp.zeros_like(near))
        total = total + next_ref[cols, :].astype(jnp.float32)
        sum_ref[cols, :] = total + over_ref[cols, :].astype(jnp.float32)
    for lanes in range(WIDE):
        cols = slice(lanes * TOK, (lanes + 1) * TOK)
        picked = sum_ref[pl.ds(lanes, 2 * SHARES, stride=WIDE), :]
        out_ref[:, cols] = picked.astype(jnp.bfloat16)


def reduce_kernel(place, came_ref, out_ref):
    total = came_ref[0].astype(jnp.float32)
    for source in range(1, SHARES):
        total = total + came_ref[source].astype(jnp.float32)
    total = total.astype(jnp.bfloat16)
    for share in range(SHARES):
        out_ref[share] = total


def finish_kernel(place, came_ref, out_ref):
    for lanes in range(WIDE):
        cols = slice(lanes * TOK, (lanes + 1) * TOK)
        out_ref[pl.ds(lanes, 2 * SHARES, stride=WIDE), :] = came_ref[:, cols].astype(jnp.float32)


def routes(count):
    across = SHARES // 2

    def pairs(moves):
        return [
            (a * SHARES + head, b * SHARES + (head ^ other))
            for a, b, other in moves
            if 0 <= b < count
            for head in range(SHARES)
        ]

    halo = pairs([(i, i + 2, across) for i in range(count)])
    mixed = pairs([(i, i + 1 + 2 * (i % 2), 0) for i in range(count)])
    back = pairs([(i, i - 2, across) for i in range(count)])
    over = pairs([(i, i - 4, 0) for i in range(1, count, 2)])
    return halo, mixed, back, over


def per_device(queries, latent_kv, grad_out, doc_start):
    tokens, _, width = queries.shape
    everyone = SEQ + HEAD
    swap = [(0, 1), (1, 0)]
    halo, mixed, back, over = routes(lax.axis_size(SEQ))
    place = lax.axis_index(SEQ).astype(jnp.int32).reshape(1)

    own = latent_kv.T
    p2 = lax.ppermute(own, everyone, halo)
    px = lax.ppermute(own, everyone, mixed)
    sw = lax.ppermute(p2, "core", swap)

    q = queries.transpose(1, 0, 2).reshape(ROWS, width)
    qt = queries.transpose(2, 1, 0).reshape(width, ROWS)
    g = grad_out.transpose(1, 0, 2).reshape(ROWS, LAT)
    doc = doc_start.astype(jnp.float32).reshape(1, tokens)

    pair = [pltpu.VMEM((width, 2 * TOK), jnp.bfloat16), pltpu.VMEM((TOK, 2 * TOK), jnp.float32)]
    half = jax.ShapeDtypeStruct((ROWS, 2 * TOK), jnp.float32)
    table = jax.ShapeDtypeStruct((ROWS, 4 * TOK), jnp.bfloat16)
    sent = jax.ShapeDtypeStruct((2, width, tokens), jnp.bfloat16)
    kept = jax.ShapeDtypeStruct((2, width, tokens), jnp.float32)
    work = 2 * ROWS * TOK * (width + LAT)
    px_now, p2_now, late = lax.optimization_barrier((px, p2, grad_out))
    gt = jnp.pad(late.transpose(2, 1, 0).reshape(LAT, ROWS), ((0, width - LAT), (0, 0)))
    scores, grads = call(near_kernel, "near", (half, half), 5, pair, work, 12)(
        place, doc, q, g, px_now, p2_now
    )
    send, probs, ds = call(attention_kernel, "attention", (sent, table, table), 9, pair, 2 * work, 20)(
        place, doc, q, qt, g, gt, scores, grads, own, sw
    )
    came = lax.ppermute(send, "core", swap)
    keep = call(keep_kernel, "keep", kept, 4, (), work, 12)(place, qt, gt, probs, ds)
    block = jax.ShapeDtypeStruct((width, tokens), jnp.bfloat16)
    flat = jax.ShapeDtypeStruct((2 * SHARES, WIDE * tokens), jnp.bfloat16)
    pieces = jax.ShapeDtypeStruct((SHARES, 2, WIDE * tokens), jnp.bfloat16)
    to_next, to_over = call(join_kernel, "join", (block, block), 2)(place, keep, came)
    ds, to_next, to_over = lax.optimization_barrier((ds, to_next, to_over))
    to_next = lax.ppermute(to_next, everyone, back)
    to_over = lax.ppermute(to_over, everyone, over)
    query_grad = query_grads(ds, own, px, p2, sw)
    to_next, to_over, query_grad = lax.optimization_barrier((to_next, to_over, query_grad))

    terms = call(
        total_kernel, "total", flat, 4, [pltpu.VMEM((width, tokens), jnp.float32)]
    )(place, keep, came, to_next, to_over)
    terms = lax.all_to_all(terms.reshape(pieces.shape), HEAD, 0, 0, tiled=True)
    terms = call(reduce_kernel, "reduce", pieces, 1)(place, terms)
    grad = lax.all_to_all(terms, HEAD, 0, 0, tiled=True)
    out = jax.ShapeDtypeStruct((width, tokens), jnp.float32)
    grad = call(finish_kernel, "finish", out, 1)(place, grad.reshape(flat.shape))
    return query_grad.transpose(2, 0, 1), grad.T


def solution(mesh):
    fine = Mesh(mesh.devices.reshape(8, 2, 2, 4, 8), ("z", "xh", "core", "xl", "y"))
    in_specs = (P(SEQ, HEAD, None), P(SEQ, None), P(SEQ, HEAD, None), P(SEQ))
    out_specs = (P(SEQ, HEAD, None), P(SEQ, None))
    return jax.shard_map(
        per_device, mesh=fine, in_specs=in_specs, out_specs=out_specs, check_vma=False
    )
```

```python
import jax
import jax.numpy as jnp
from jax import lax
from jax.experimental import pallas as pl
from jax.experimental.pallas import tpu as pltpu
from jax.sharding import Mesh
from jax.sharding import PartitionSpec as P

LAT = 512
KVW = 576
TOK = 128
HEADS = 4
ROWS = TOK * HEADS
PART = 72
SHARES = 32
WIDE = KVW // (2 * SHARES)
SEQ = ("z", "xh", "core")
HEAD = ("xl", "y")

softmax_scale = 192.0 ** (-0.5)
lowest = -1e30
whole = pl.BlockSpec(memory_space=pltpu.VMEM)
scalars = pl.BlockSpec(memory_space=pltpu.SMEM)


def f32_dot(a, b):
    return jnp.dot(a, b, preferred_element_type=jnp.float32)


def load_pair(place, doc_ref, backs, blocks, kv_ref, bias_ref):
    seq = place[0]
    first = jnp.broadcast_to(doc_ref[...], (TOK, TOK)).T
    row = lax.broadcasted_iota(jnp.int32, (TOK, TOK), 0)
    lane = lax.broadcasted_iota(jnp.int32, (TOK, TOK), 1)
    for slot, (back, ref) in enumerate(zip(backs, blocks)):
        cols = slice(slot * TOK, (slot + 1) * TOK)
        kv_ref[:, cols] = ref[...]
        key = lane + (seq - back) * TOK
        seen = (key <= row + seq * TOK) & (key.astype(jnp.float32) >= first)
        bias_ref[:, cols] = jnp.where(seen, 0.0, lowest)


def near_kernel(
    place, doc_ref, q_ref, g_ref, px_ref, p2_ref, score_ref, grad_ref, gt_ref, kv_ref, bias_ref
):
    core = lax.rem(place[0], 2)
    load_pair(place, doc_ref, (3 - 2 * core, 2), (px_ref, p2_ref), kv_ref, bias_ref)
    for head in range(HEADS):
        rows = slice(head * TOK, (head + 1) * TOK)
        score_ref[rows, :] = f32_dot(q_ref[rows, :], kv_ref[...]) * softmax_scale + bias_ref[...]
        grad_ref[rows, :] = f32_dot(g_ref[rows, :], kv_ref[:LAT, :])
        gt_ref[:LAT, rows] = g_ref[rows, :].T
    gt_ref[LAT:, :] = jnp.zeros((KVW - LAT, ROWS), jnp.bfloat16)


def add_terms(qt_ref, gt_ref, ds_ref, p_ref, part, lanes):
    cols = slice(part * PART, (part + 1) * PART)
    term = f32_dot(qt_ref[cols, :], ds_ref[:, lanes]) * softmax_scale
    return cols, term + f32_dot(gt_ref[cols, :], p_ref[:, lanes])


def attention_kernel(
    place, doc_ref, q_ref, qt_ref, g_ref, gt_ref, score_ref, grad_ref, own_ref, sw_ref,
    send_ref, p_ref, ds_ref, kv_ref, bias_ref,
):
    core = lax.rem(place[0], 2)
    load_pair(place, doc_ref, (0, 1 + 2 * core), (own_ref, sw_ref), kv_ref, bias_ref)
    for head in range(HEADS):
        rows = slice(head * TOK, (head + 1) * TOK)
        far = f32_dot(q_ref[rows, :], kv_ref[...]) * softmax_scale + bias_ref[...]
        far_grads = f32_dot(g_ref[rows, :], kv_ref[:LAT, :])
        near, near_grads = score_ref[rows, :], grad_ref[rows, :]
        top = jnp.max(jnp.maximum(near, far), axis=1, keepdims=True)
        near, far = jnp.exp(near - top), jnp.exp(far - top)
        inverse = 1.0 / jnp.sum(near + far, axis=1, keepdims=True)
        delta = jnp.sum(near * near_grads + far * far_grads, axis=1, keepdims=True) * inverse
        for half, (exps, grads) in enumerate(((near, near_grads), (far, far_grads))):
            probs = exps * inverse
            for slot in range(2):
                mine = slice(slot * TOK, (slot + 1) * TOK)
                place_at = ((0, 3), (2, 1))[half][slot]
                lanes = slice(place_at * TOK, (place_at + 1) * TOK)
                p_ref[rows, lanes] = probs[:, mine].astype(jnp.bfloat16)
                ds_ref[rows, lanes] = (probs[:, mine] * (grads[:, mine] - delta)).astype(
                    jnp.bfloat16
                )
    for part in range(KVW // PART):
        cols, term = add_terms(qt_ref, gt_ref, ds_ref, p_ref, part, slice(0, 2 * TOK))
        send_ref[0, cols, :] = term[:, :TOK].astype(jnp.bfloat16)
        send_ref[1, cols, :] = term[:, TOK:].astype(jnp.bfloat16)


def keep_kernel(place, qt_ref, gt_ref, p_ref, ds_ref, keep_ref):
    for part in range(KVW // PART):
        cols, term = add_terms(qt_ref, gt_ref, ds_ref, p_ref, part, slice(2 * TOK, 4 * TOK))
        keep_ref[0, cols, :] = term[:, :TOK]
        keep_ref[1, cols, :] = term[:, TOK:]


def queries_kernel(ds_ref, own_ref, px_ref, p2_ref, sw_ref, out_ref, kv_ref):
    for slot, ref in enumerate((px_ref, sw_ref, own_ref, p2_ref)):
        kv_ref[:, slot * TOK : (slot + 1) * TOK] = ref[...]
    for head in range(HEADS):
        rows = slice(head * TOK, (head + 1) * TOK)
        total = lax.dot_general(
            kv_ref[...], ds_ref[rows, :], (((1,), (1,)), ((), ())), preferred_element_type=jnp.float32
        )
        out_ref[head] = (total * softmax_scale).astype(jnp.bfloat16)


def query_grads(ds, own, px, p2, sw):
    return pl.pallas_call(
        queries_kernel,
        out_shape=jax.ShapeDtypeStruct((HEADS, KVW, TOK), jnp.bfloat16),
        in_specs=[whole] * 5,
        out_specs=whole,
        scratch_shapes=[pltpu.VMEM((KVW, 4 * TOK), jnp.bfloat16)],
        cost_estimate=pl.CostEstimate(
            flops=2 * ROWS * 4 * TOK * KVW, bytes_accessed=2 << 20, transcendentals=0
        ),
        compiler_params=pltpu.CompilerParams(vmem_limit_bytes=12 << 20),
        name="query_grads",
    )(ds, own, px, p2, sw)


def call(kernel, name, out_shape, count, scratch=(), macs=1 << 18, limit=8):
    outs = out_shape if isinstance(out_shape, tuple) else (out_shape,)
    specs = (whole,) * len(outs)
    return pl.pallas_call(
        kernel,
        out_shape=out_shape,
        in_specs=[scalars] + [whole] * count,
        out_specs=specs if isinstance(out_shape, tuple) else whole,
        scratch_shapes=list(scratch),
        cost_estimate=pl.CostEstimate(flops=2 * macs, bytes_accessed=1 << 20, transcendentals=0),
        compiler_params=pltpu.CompilerParams(vmem_limit_bytes=limit << 20),
        name=name,
    )


def join_kernel(place, keep_ref, came_ref, next_ref, over_ref):
    odd = lax.rem(place[0], 2) == 1
    for part in range(KVW // PART):
        cols = slice(part * PART, (part + 1) * PART)
        side = came_ref[1, cols, :].astype(jnp.float32)
        next_ref[cols, :] = (keep_ref[1, cols, :] + side).astype(jnp.bfloat16)
        far = came_ref[0, cols, :].astype(jnp.float32)
        over_ref[cols, :] = jnp.where(odd, far, jnp.zeros_like(far)).astype(jnp.bfloat16)


def total_kernel(place, keep_ref, came_ref, next_ref, over_ref, out_ref, sum_ref):
    even = lax.rem(place[0], 2) == 0
    for part in range(KVW // PART):
        cols = slice(part * PART, (part + 1) * PART)
        near = came_ref[0, cols, :].astype(jnp.float32)
        total = keep_ref[0, cols, :] + jnp.where(even, near, jnp.zeros_like(near))
        total = total + next_ref[cols, :].astype(jnp.float32)
        sum_ref[cols, :] = total + over_ref[cols, :].astype(jnp.float32)
    for lanes in range(WIDE):
        cols = slice(lanes * TOK, (lanes + 1) * TOK)
        picked = sum_ref[pl.ds(lanes, 2 * SHARES, stride=WIDE), :]
        out_ref[:, cols] = picked.astype(jnp.bfloat16)


def reduce_kernel(place, came_ref, out_ref):
    total = came_ref[0].astype(jnp.float32)
    for source in range(1, SHARES):
        total = total + came_ref[source].astype(jnp.float32)
    total = total.astype(jnp.bfloat16)
    for share in range(SHARES):
        out_ref[share] = total


def finish_kernel(place, came_ref, out_ref):
    for lanes in range(WIDE):
        cols = slice(lanes * TOK, (lanes + 1) * TOK)
        out_ref[pl.ds(lanes, 2 * SHARES, stride=WIDE), :] = came_ref[:, cols].astype(jnp.float32)


def routes(count):
    across = SHARES // 2

    def pairs(moves):
        return [
            (a * SHARES + head, b * SHARES + (head ^ other))
            for a, b, other in moves
            if 0 <= b < count
            for head in range(SHARES)
        ]

    halo = pairs([(i, i + 2, across) for i in range(count)])
    mixed = pairs([(i, i + 1 + 2 * (i % 2), 0) for i in range(count)])
    back = pairs([(i, i - 2, across) for i in range(count)])
    over = pairs([(i, i - 4, 0) for i in range(1, count, 2)])
    return halo, mixed, back, over


def per_device(queries, latent_kv, grad_out, doc_start):
    tokens, _, width = queries.shape
    everyone = SEQ + HEAD
    swap = [(0, 1), (1, 0)]
    halo, mixed, back, over = routes(lax.axis_size(SEQ))
    place = lax.axis_index(SEQ).astype(jnp.int32).reshape(1)

    own = latent_kv.T
    p2 = lax.ppermute(own, everyone, halo)
    px = lax.ppermute(own, everyone, mixed)
    sw = lax.ppermute(p2, "core", swap)

    q = queries.transpose(1, 0, 2).reshape(ROWS, width)
    qt = queries.transpose(2, 1, 0).reshape(width, ROWS)
    g = grad_out.transpose(1, 0, 2).reshape(ROWS, LAT)
    doc = doc_start.astype(jnp.float32).reshape(1, tokens)

    pair = [pltpu.VMEM((width, 2 * TOK), jnp.bfloat16), pltpu.VMEM((TOK, 2 * TOK), jnp.float32)]
    half = jax.ShapeDtypeStruct((ROWS, 2 * TOK), jnp.float32)
    table = jax.ShapeDtypeStruct((ROWS, 4 * TOK), jnp.bfloat16)
    sent = jax.ShapeDtypeStruct((2, width, tokens), jnp.bfloat16)
    kept = jax.ShapeDtypeStruct((2, width, tokens), jnp.float32)
    work = 2 * ROWS * TOK * (width + LAT)
    px_now, p2_now = lax.optimization_barrier((px, p2))
    turned = jax.ShapeDtypeStruct((width, ROWS), jnp.bfloat16)
    scores, grads, gt = call(near_kernel, "near", (half, half, turned), 5, pair, work, 12)(
        place, doc, q, g, px_now, p2_now
    )
    send, probs, ds = call(attention_kernel, "attention", (sent, table, table), 9, pair, 2 * work, 20)(
        place, doc, q, qt, g, gt, scores, grads, own, sw
    )
    came = lax.ppermute(send, "core", swap)
    keep = call(keep_kernel, "keep", kept, 4, (), work, 12)(place, qt, gt, probs, ds)
    block = jax.ShapeDtypeStruct((width, tokens), jnp.bfloat16)
    flat = jax.ShapeDtypeStruct((2 * SHARES, WIDE * tokens), jnp.bfloat16)
    pieces = jax.ShapeDtypeStruct((SHARES, 2, WIDE * tokens), jnp.bfloat16)
    to_next, to_over = call(join_kernel, "join", (block, block), 2)(place, keep, came)
    ds, to_next, to_over = lax.optimization_barrier((ds, to_next, to_over))
    to_next = lax.ppermute(to_next, everyone, back)
    to_over = lax.ppermute(to_over, everyone, over)
    query_grad = query_grads(ds, own, px, p2, sw)
    to_next, to_over, query_grad = lax.optimization_barrier((to_next, to_over, query_grad))

    terms = call(
        total_kernel, "total", flat, 4, [pltpu.VMEM((width, tokens), jnp.float32)]
    )(place, keep, came, to_next, to_over)
    terms = lax.all_to_all(terms.reshape(pieces.shape), HEAD, 0, 0, tiled=True)
    terms = call(reduce_kernel, "reduce", pieces, 1)(place, terms)
    grad = lax.all_to_all(terms, HEAD, 0, 0, tiled=True)
    out = jax.ShapeDtypeStruct((width, tokens), jnp.float32)
    grad = call(finish_kernel, "finish", out, 1)(place, grad.reshape(flat.shape))
    return query_grad.transpose(2, 0, 1), grad.T


def solution(mesh):
    fine = Mesh(mesh.devices.reshape(8, 2, 2, 4, 8), ("z", "xh", "core", "xl", "y"))
    in_specs = (P(SEQ, HEAD, None), P(SEQ, None), P(SEQ, HEAD, None), P(SEQ))
    out_specs = (P(SEQ, HEAD, None), P(SEQ, None))
    return jax.shard_map(
        per_device, mesh=fine, in_specs=in_specs, out_specs=out_specs, check_vma=False
    )
```
